32 devices in a mesh: batch: 2 (over x), seq: 16 (over z, y, core).
Axes of the slice: x: 2, y: 2, z: 4, core: 2. Of those that a mesh axis runs over, the one named last changes fastest.
Arguments:
- layer_input: bfloat16 [4, 2048, 768], P('batch', 'seq'), may hold values from -10 to 10
- query_weight: bfloat16 [768, 768], P(('batch', 'seq')), may hold values from -0.21875 to 0.21875
- key_weight: bfloat16 [768, 768], P(('batch', 'seq')), may hold values from -0.21875 to 0.21875
- value_weight: bfloat16 [768, 768], P(('batch', 'seq')), may hold values from -0.21875 to 0.21875
- output_weight: bfloat16 [768, 768], P(('batch', 'seq')), may hold values from -0.21875 to 0.21875
- up_weight: bfloat16 [768, 3072], P(('batch', 'seq')), may hold values from -0.21875 to 0.21875
- down_weight: bfloat16 [3072, 768], P(('batch', 'seq')), may hold values from -0.109375 to 0.109375
- query_bias: bfloat16 [768], P(('batch', 'seq')), may hold values from -3 to 3
- value_bias: bfloat16 [768], P(('batch', 'seq')), may hold values from -3 to 3
- output_bias: bfloat16 [768], P(('batch', 'seq')), may hold values from -3 to 3
- up_bias: bfloat16 [3072], P(('batch', 'seq')), may hold values from -3 to 3
- down_bias: bfloat16 [768], P(('batch', 'seq')), may hold values from -3 to 3
- first_gain: bfloat16 [768], P(('batch', 'seq')), may hold values from 0.25 to 1.75
- first_shift: bfloat16 [768], P(('batch', 'seq')), may hold values from -2 to 2
- second_gain: bfloat16 [768], P(('batch', 'seq')), may hold values from 0.25 to 1.75
- second_shift: bfloat16 [768], P(('batch', 'seq')), may hold values from -2 to 2
- mixing_taps: bfloat16 [12, 33], replicated, may hold values from -1 to 1
- output_cotangent: bfloat16 [4, 2048, 768], P('batch', 'seq'), may hold values from -6 to 6
Outputs:
- layer_output: bfloat16 [4, 2048, 768], P('batch', 'seq')
- input_gradient: float32 [4, 2048, 768], P('batch', 'seq')
- query_weight_gradient: float32 [768, 768], P(('batch', 'seq'))
- key_weight_gradient: float32 [768, 768], P(('batch', 'seq'))
- value_weight_gradient: float32 [768, 768], P(('batch', 'seq'))
- output_weight_gradient: float32 [768, 768], P(('batch', 'seq'))
- up_weight_gradient: float32 [768, 3072], P(('batch', 'seq'))
- down_weight_gradient: float32 [3072, 768], P(('batch', 'seq'))
- query_bias_gradient: float32 [768], P(('batch', 'seq'))
- value_bias_gradient: float32 [768], P(('batch', 'seq'))
- output_bias_gradient: float32 [768], P(('batch', 'seq'))
- up_bias_gradient: float32 [3072], P(('batch', 'seq'))
- down_bias_gradient: float32 [768], P(('batch', 'seq'))
- first_gain_gradient: float32 [768], P(('batch', 'seq'))
- first_shift_gradient: float32 [768], P(('batch', 'seq'))
- second_gain_gradient: float32 [768], P(('batch', 'seq'))
- second_shift_gradient: float32 [768], P(('batch', 'seq'))
- mixing_taps_gradient: float32 [12, 33], replicated
- pinv_error: float32 [], replicated
The draws below stay inside these ranges and needn't reach their ends.
All inputs are finite; a program needn't handle non-finite values.
Results may differ from the reference program's by a relative error of at most 0.022.
The reference program's roundings to bfloat16 on the way count: a program that leaves them out, or rounds other values in their place, can miss the bound.
Values may be sent and summed in bfloat16 or wider, within the bound.
A program may use at most 192 MiB of HBM per device.

```python
import jax
import jax.numpy as jnp
from jax import lax

HEADS = 12
HEAD_DIM = 64
FF = 3072
LANDMARKS = 64
KERNEL = 33
NEWTON = 6
D = 768
RIM = 16
LEN = 2048
SEQS = 4
SEG = 32


def draw_layer_input(key, part):
    noise_key, common_key = jax.random.split(key)
    noise = jax.random.normal(noise_key, (SEQS, LEN, D), jnp.float32)
    common = jax.random.normal(common_key, (SEQS, LANDMARKS, 1, D), jnp.float32)
    common = jnp.broadcast_to(common, (SEQS, LANDMARKS, SEG, D)).reshape(SEQS, LEN, D)
    ramp = 0.8 + 1.6 * jnp.arange(SEQS, dtype=jnp.float32) / max(SEQS - 1, 1)
    values = ramp[:, None, None] * (0.6 * noise + 0.8 * common)
    return jnp.clip(values, -10.0, 10.0).astype(jnp.bfloat16)


def shard_levels(rng, dims, pieces, least, top_value):
    level = 1.0
    for axis_at, blocks in pieces:
        draws = jax.random.uniform(jax.random.fold_in(jax.random.fold_in(rng, 6), axis_at), (blocks,), jnp.float32, least / len(pieces), top_value / len(pieces))
        level = level * jnp.repeat(jnp.exp(draws), dims[axis_at] // blocks).reshape((-1,) + (1,) * (len(dims) - 1 - axis_at))
    return level


def bell_draw(rng, dims, deviation, bound, shards=(), kind=jnp.bfloat16):
    drawn = jax.random.normal(rng, dims, jnp.float32) * deviation
    if len(shards) > 0:
        drawn = shard_levels(rng, dims, shards, -0.22, 0.18) * drawn
    return jnp.clip(drawn, min=-bound, max=bound).astype(kind)


def setup_inputs(seed: int = 0) -> dict:
    streams_of = jax.random.split(jax.random.key(seed), 19)
    layer_input = draw_layer_input(jax.random.fold_in(streams_of[18], 71), 0)
    query_weight = bell_draw(streams_of[1], (D, D), D ** -0.5, 0.21875, ((0, 32),))
    key_weight = bell_draw(streams_of[2], (D, D), D ** -0.5, 0.21875, ((0, 32),))
    value_weight = bell_draw(streams_of[3], (D, D), D ** -0.5, 0.21875, ((0, 32),))
    output_weight = bell_draw(streams_of[4], (D, D), D ** -0.5, 0.21875, ((0, 32),))
    up_weight = bell_draw(streams_of[5], (D, FF), D ** -0.5, 0.21875, ((0, 32),))
    down_weight = bell_draw(streams_of[6], (FF, D), FF ** -0.5, 0.109375, ((0, 32),))
    query_bias = bell_draw(streams_of[7], (D,), 0.5, 3.0, ((0, 32),))
    value_bias = bell_draw(streams_of[8], (D,), 0.5, 3.0, ((0, 32),))
    output_bias = bell_draw(streams_of[9], (D,), 0.5, 3.0, ((0, 32),))
    up_bias = bell_draw(streams_of[10], (FF,), 0.5, 3.0, ((0, 32),))
    down_bias = bell_draw(streams_of[11], (D,), 0.5, 3.0, ((0, 32),))
    first_gain = jnp.clip(1.0 + 0.15 * jax.random.normal(streams_of[12], (D,), jnp.float32), 0.25, 1.75).astype(jnp.bfloat16)
    first_shift = bell_draw(streams_of[13], (D,), 0.3, 2.0, ((0, 32),))
    second_gain = jnp.clip(1.0 + 0.15 * jax.random.normal(streams_of[14], (D,), jnp.float32), 0.25, 1.75).astype(jnp.bfloat16)
    second_shift = bell_draw(streams_of[15], (D,), 0.3, 2.0, ((0, 32),))
    mixing_taps = bell_draw(streams_of[16], (HEADS, KERNEL), KERNEL ** -0.5, 1.0)
    output_cotangent = bell_draw(streams_of[17], (SEQS, LEN, D), 1.0, 6.0, ((0, 2), (1, 16)))
    return {"layer_input": layer_input, "query_weight": query_weight, "key_weight": key_weight, "value_weight": value_weight, "output_weight": output_weight, "up_weight": up_weight, "down_weight": down_weight, "query_bias": query_bias, "value_bias": value_bias, "output_bias": output_bias, "up_bias": up_bias, "down_bias": down_bias, "first_gain": first_gain, "first_shift": first_shift, "second_gain": second_gain, "second_shift": second_shift, "mixing_taps": mixing_taps, "output_cotangent": output_cotangent}


highest_precision = lax.Precision.HIGHEST

@jax.custom_vjp
def low(v):
    return lax.optimization_barrier(v.astype(jnp.bfloat16)).astype(jnp.float32)

@jax.custom_vjp
def low_back(v):
    return v

def low_keep(v):
    return (low(v), None)

def low_pass(kept, grad):
    return (grad,)

def back_keep(v):
    return (v, None)

def back_low(kept, grad):
    return (low(grad),)
low.defvjp(low_keep, low_pass)
low_back.defvjp(back_keep, back_low)

def layer_norm(rows, gain, shift):
    centre = rows - lax.optimization_barrier(jnp.mean(rows, axis=-1, keepdims=True))
    spread = lax.optimization_barrier(jnp.mean(centre * centre, axis=-1, keepdims=True))
    return centre * lax.rsqrt(spread + 1e-05) * gain + shift

def split_heads(matrix):
    return matrix.reshape(matrix.shape[:-1] + (HEADS, HEAD_DIM))

def pseudo_inverse(landmark_kernel_matrix):
    column_top = lax.optimization_barrier(jnp.max(lax.optimization_barrier(jnp.sum(landmark_kernel_matrix, axis=-2)), axis=-1))
    row_top = lax.optimization_barrier(jnp.max(lax.optimization_barrier(jnp.sum(landmark_kernel_matrix, axis=-1)), axis=-1))
    approx = jnp.swapaxes(landmark_kernel_matrix, -1, -2) / (column_top * row_top)[..., None, None]
    ident = jnp.eye(landmark_kernel_matrix.shape[-1], dtype=jnp.float32)
    for turn_index in range(NEWTON):
        product = jnp.matmul(landmark_kernel_matrix, approx, precision=highest_precision)
        inner = 7.0 * ident - product
        inner = 15.0 * ident - jnp.matmul(product, inner, precision=highest_precision)
        inner = 13.0 * ident - jnp.matmul(product, inner, precision=highest_precision)
        approx = 0.25 * jnp.matmul(approx, inner, precision=highest_precision)
    return approx

def product(left, right):
    return jnp.dot(left, right, precision=highest_precision, preferred_element_type=jnp.float32)

def forward(rows, weights):
    query_weight, key_weight, value_weight, output_weight, up_weight, down_weight, query_bias, value_bias, output_bias, up_bias, down_bias, first_gain, first_shift, second_gain, second_shift, mixing_taps = weights
    queries = low_back(product(rows, query_weight) + query_bias)
    key_rows = low_back(product(rows, key_weight))
    value_rows = low(low_back(product(rows, value_weight) + value_bias))
    mark_query = low(lax.optimization_barrier(jnp.mean(queries.reshape(LANDMARKS, SEG, D), axis=1)))
    mark_key = low(lax.optimization_barrier(jnp.mean(key_rows.reshape(LANDMARKS, SEG, D), axis=1)))
    scale = HEAD_DIM ** (-0.25)
    query_head_rows = split_heads(queries) * scale
    key_head_rows = split_heads(key_rows) * scale
    landmark_query_heads = split_heads(mark_query) * scale
    landmark_key_heads = split_heads(mark_key) * scale
    value_head_rows = split_heads(value_rows)
    nearby_part = jax.nn.softmax(jnp.einsum('axy,uxy->xau', query_head_rows, landmark_key_heads, precision=highest_precision), axis=-1)
    landmark_kernel_matrix = jax.nn.softmax(jnp.einsum('rlt,slt->lrs', landmark_query_heads, landmark_key_heads, precision=highest_precision), axis=-1)
    distant_part = jax.nn.softmax(jnp.einsum('gcf,xcf->cgx', landmark_query_heads, key_head_rows, precision=highest_precision), axis=-1)
    distant_values = jnp.einsum('opk,koa->opa', distant_part, value_head_rows, precision=highest_precision)
    inverse = pseudo_inverse(landmark_kernel_matrix)
    mixing_result = jnp.matmul(inverse, distant_values, precision=highest_precision)
    attended_output = jnp.einsum('zau,zus->azs', nearby_part, mixing_result, precision=highest_precision)
    padded = jnp.pad(value_head_rows, ((RIM, RIM), (0, 0), (0, 0)))
    for tap_index in range(KERNEL):
        attended_output = attended_output + mixing_taps[:, tap_index][:, None] * padded[tap_index:tap_index + LEN]
    attention = low(attended_output.reshape(LEN, D))
    resid_first = rows + low_back(product(attention, output_weight) + output_bias)
    hidden = layer_norm(resid_first, first_gain, first_shift)
    upper = low_back(product(low(hidden), up_weight) + up_bias)
    lower = low_back(product(low(jax.nn.gelu(upper, approximate=False)), down_weight) + down_bias)
    normed = layer_norm(hidden + lower, second_gain, second_shift)
    ident = jnp.eye(LANDMARKS, dtype=jnp.float32)
    defect = ident - jnp.matmul(landmark_kernel_matrix, inverse, precision=highest_precision)
    error = jnp.sum(jnp.sqrt(lax.optimization_barrier(jnp.sum(defect * defect, axis=(-2, -1)))))
    return (normed, error)

def reference(layer_input, query_weight, key_weight, value_weight, output_weight, up_weight, down_weight, query_bias, value_bias, output_bias, up_bias, down_bias, first_gain, first_shift, second_gain, second_shift, mixing_taps, output_cotangent):
    weights = tuple((item.astype(jnp.float32) for item in (query_weight, key_weight, value_weight, output_weight, up_weight, down_weight, query_bias, value_bias, output_bias, up_bias, down_bias, first_gain, first_shift, second_gain, second_shift, mixing_taps)))

    def one_sequence(totals, pair):
        rows, cotangent = pair
        normed, back_fn, error = jax.vjp(forward, rows.astype(jnp.float32), weights, has_aux=True)
        delta_rows, delta_weights = back_fn(cotangent.astype(jnp.float32))
        totals = jax.tree.map(jnp.add, totals, delta_weights)
        return (totals, (normed.astype(jnp.bfloat16), delta_rows, error))
    zeros = jax.tree.map(jnp.zeros_like, weights)
    totals, (outputs, deltas, errors) = lax.scan(one_sequence, zeros, (layer_input, output_cotangent))
    pinv_error = jnp.sum(errors) / (SEQS * HEADS)
    return (outputs, deltas, totals[0], totals[1], totals[2], totals[3], totals[4], totals[5], totals[6], totals[7], totals[8], totals[9], totals[10], totals[11], totals[12], totals[13], totals[14], totals[15], pinv_error)
```

```python
from functools import partial

import jax
import jax.numpy as jnp
from jax import lax
from jax.experimental import pallas as pl
from jax.experimental.pallas import tpu as pltpu
from jax.sharding import PartitionSpec as P

MESH = pl.DeviceIdType.MESH
BATCH, SEQ = "batch", "seq"
BOTH = (BATCH, SEQ)
ROWS, SPREAD, TOKENS = P(BOTH, None), P(BOTH), P(BATCH, SEQ, None)
GATHER, SCATTER, NEXT, LAST = range(4)
ALL = slice(None)
LAG = 1


def grid_of(batch, seq):
    mid = 2 if seq < 32 else 4
    return batch, seq // (2 * mid), mid, 2


class Grid:
    def __init__(self, batch, seq):
        self.sizes = dict(zip("xzyc", grid_of(batch, seq)))
        s = lax.axis_index(SEQ)
        ny, nc = self.sizes["y"], self.sizes["c"]
        self.at = {"x": lax.axis_index(BATCH), "z": s // (ny * nc), "y": (s // nc) % ny, "c": s % nc}

    def device(self, at):
        return (at["x"], (at["z"] * self.sizes["y"] + at["y"]) * self.sizes["c"] + at["c"])

    def others(self, axis):
        size = self.sizes[axis]
        return [(step, lax.rem(self.at[axis] + step, size)) for step in range(1, size)]

    def moved(self, axis, other):
        return self.device({**self.at, axis: other})

    def greet(self):
        barrier = pltpu.get_barrier_semaphore()
        count = 0
        for axis in "zxyc":
            for _, other in self.others(axis):
                pl.semaphore_signal(barrier, inc=1, device_id=self.moved(axis, other), device_id_type=MESH)
                count += 1
        pl.semaphore_wait(barrier, count)

    def block(self, whole):
        return tuple(ALL if axis in whole else self.at[axis] for axis in "xzyc")


def gather_kernel(batch, seq, parts, orders, unit, n_in, *refs):
    ins, outs = refs[:n_in], refs[n_in : 2 * n_in]
    send_sem, recv_sem, own_sem = refs[2 * n_in :]
    g = Grid(batch, seq)
    g.greet()
    count = len(parts)
    copies = {}

    def view(part, whole):
        index, rows, cols = parts[part]
        return outs[index].at[g.block(whole) + (rows, cols)]

    def send(part, stage, axis, source, target):
        started = []
        for step, other in g.others(axis):
            copy = pltpu.make_async_remote_copy(
                src_ref=source,
                dst_ref=target,
                send_sem=send_sem.at[part, stage, step - 1],
                recv_sem=recv_sem.at[part, stage, step - 1],
                device_id=g.moved(axis, other),
                device_id_type=MESH,
            )
            copy.start()
            started.append(copy)
        copies[part, stage] = started

    def arrive(part, stage):
        for copy in copies[part, stage]:
            copy.wait_recv()

    def begin(part):
        index, rows, cols = parts[part]
        source = ins[index].at[rows, cols]
        own = pltpu.make_async_copy(source, view(part, ""), own_sem.at[part])
        own.start()
        copies[part, "own"] = own
        send(part, 0, "z", source, view(part, ""))

    def spread(stage):
        def run(part):
            axes = ("z",) + tuple(orders[part]) + ("c",)
            if stage == 1:
                copies[part, "own"].wait()
            arrive(part, stage - 1)
            if stage < 4:
                held = view(part, axes[:stage])
                send(part, stage, axes[stage], held, held)
        return run

    units = [range(at, min(at + unit, count)) for at in range(0, count, unit)]
    stages = [begin] + [spread(stage) for stage in (1, 2, 3, 4)]
    for turn in range(len(units) + 4 * LAG):
        for lag, stage in enumerate(stages):
            if 0 <= turn - lag * LAG < len(units):
                for part in units[turn - lag * LAG]:
                    stage(part)
    for part in range(count):
        for stage in range(4):
            for copy in copies[part, stage]:
                copy.wait_send()


def gather_weights(batch, seq, shards, parts, orders, unit, collective_id):
    sizes = grid_of(batch, seq)
    n, count, most = len(shards), len(parts), max(sizes) - 1
    return pl.pallas_call(
        partial(gather_kernel, batch, seq, parts, orders, unit, n),
        out_shape=[jax.ShapeDtypeStruct(sizes + s.shape, s.dtype) for s in shards],
        in_specs=[pl.BlockSpec(memory_space=pltpu.VMEM)] * n,
        out_specs=[pl.BlockSpec(memory_space=pl.ANY)] * n,
        scratch_shapes=[
            pltpu.SemaphoreType.DMA((count, 4, most)),
            pltpu.SemaphoreType.DMA((count, 4, most)),
            pltpu.SemaphoreType.DMA((count,)),
        ],
        compiler_params=pltpu.CompilerParams(collective_id=collective_id, has_side_effects=True),
        name="gather_weights",
    )(*shards)


def scatter_kernel(batch, seq, parts, orders, unit, n_in, *refs):
    ins, outs = refs[:n_in], refs[n_in : 2 * n_in]
    own_sem, send_sem, recv_sem = refs[-3:]
    scratch = refs[2 * n_in : -3]
    g = Grid(batch, seq)
    g.greet()
    count = len(parts)
    copies = {}
    shapes = [part_shape(ins, part) for part in parts]
    groups = sorted(set(shapes), key=shapes.index)
    held, from_core, far, from_near, from_line = ([None] * count for _ in range(5))
    for at, shape in enumerate(groups):
        members = [part for part in range(count) if shapes[part] == shape]
        buffers = scratch[6 * at : 6 * at + 6]
        for rank, part in enumerate(members):
            far_rank = [p for p in members if orders[p] == orders[part]].index(part)
            held[part], from_core[part] = buffers[0].at[rank], buffers[1].at[rank]
            far[part] = (buffers[2] if orders[part][1] == "y" else buffers[3]).at[far_rank]
            from_near[part], from_line[part] = buffers[4].at[rank], buffers[5].at[rank]

    def source(part, core):
        index, rows, cols = parts[part]
        return ins[index].at[ALL, ALL, ALL, core, rows, cols]

    def mine(part, whole, **moved):
        at = {**g.at, **moved}
        return held[part].at[tuple(ALL if axis in whole else at[axis] for axis in "xzy")]

    def send(part, stage, axis, step, other, src, dst):
        copy = pltpu.make_async_remote_copy(
            src_ref=src,
            dst_ref=dst,
            send_sem=send_sem.at[part, stage, step - 1],
            recv_sem=recv_sem.at[part, stage, step - 1],
            device_id=g.moved(axis, other),
            device_id_type=MESH,
        )
        copy.start()
        copies.setdefault((part, stage), []).append(copy)

    def accumulate(into, others):
        lead = into.shape[:-2]
        total = 1
        for size in lead:
            total *= size

        def step(i, carry):
            at = []
            for size in reversed(lead):
                at.insert(0, i % size)
                i = i // size
            at = tuple(at)
            value = into[at].astype(jnp.float32)
            for other in others:
                value += other[at].astype(jnp.float32)
            into[at] = value.astype(into.dtype)
            return carry

        lax.fori_loop(0, total, step, 0)

    def begin(part):
        own = pltpu.make_async_copy(source(part, g.at["c"]), held[part], own_sem.at[part])
        own.start()
        copies[part, "own"] = own
        for step, other in g.others("c"):
            send(part, 0, "c", step, other, source(part, other), from_core[part])

    def arrive(part, stage):
        for copy in copies[part, stage]:
            copy.wait_recv()

    def reduce_core(part):
        copies[part, "own"].wait()
        arrive(part, 0)
        accumulate(held[part], [from_core[part]])
        axis = orders[part][1]
        whole = "xzy".replace(axis, "")
        for step, other in g.others(axis):
            send(part, 1, axis, step, other, mine(part, whole, **{axis: other}), far[part].at[step - 1])

    def reduce_far(part):
        arrive(part, 1)
        near, axis = orders[part]
        accumulate(
            mine(part, "xzy".replace(axis, "")), [far[part].at[step - 1] for step, _ in g.others(axis)]
        )
        for step, other in g.others(near):
            send(part, 2, near, step, other, mine(part, "z", **{near: other}), from_near[part].at[step - 1])

    def reduce_near(part):
        arrive(part, 2)
        near = orders[part][0]
        accumulate(mine(part, "z"), [from_near[part].at[step - 1] for step, _ in g.others(near)])
        for step, other in g.others("z"):
            send(part, 3, "z", step, other, mine(part, "", z=other), from_line[part].at[step - 1])

    def reduce_line(part):
        arrive(part, 3)
        index, rows, cols = parts[part]
        value = mine(part, "")[...].astype(jnp.float32)
        for step, _ in g.others("z"):
            value += from_line[part][step - 1].astype(jnp.float32)
        outs[index][rows, cols] = value

    units = [range(at, min(at + unit, count)) for at in range(0, count, unit)]
    stages = [begin, reduce_core, reduce_far, reduce_near, reduce_line]
    for turn in range(len(units) + 4 * LAG):
        for lag, stage in enumerate(stages):
            if 0 <= turn - lag * LAG < len(units):
                for part in units[turn - lag * LAG]:
                    stage(part)
    for part in range(count):
        for stage in range(4):
            for copy in copies[part, stage]:
                copy.wait_send()


def part_shape(arrays, part):
    index, rows, cols = part
    array = arrays[index]
    spans = [len(range(*span.indices(size))) for span, size in zip((rows, cols), array.shape[-2:])]
    return (*spans, array.dtype)


def scatter_grads(batch, seq, grads, parts, orders, unit, collective_id):
    sizes = nx, nz, ny, nc = grid_of(batch, seq)
    n, count, most = len(grads), len(parts), max(sizes) - 1
    shapes = [part_shape(grads, part) for part in parts]
    scratch = []
    for shape in sorted(set(shapes), key=shapes.index):
        members = [part for part in range(count) if shapes[part] == shape]
        rows, cols, kind = shape
        ways = [orders[part] for part in members]
        total = len(members)
        scratch += [
            pltpu.VMEM((total, nx, nz, ny, rows, cols), kind),
            pltpu.VMEM((total, nx, nz, ny, rows, cols), kind),
            pltpu.VMEM((max(1, ways.count("xy")), ny - 1, nx, nz, rows, cols), kind),
            pltpu.VMEM((max(1, ways.count("yx")), nx - 1, nz, ny, rows, cols), kind),
            pltpu.VMEM((total, max(nx, ny) - 1, nz, rows, cols), kind),
            pltpu.VMEM((total, nz - 1, rows, cols), kind),
        ]
    return pl.pallas_call(
        partial(scatter_kernel, batch, seq, parts, orders, unit, n),
        out_shape=[jax.ShapeDtypeStruct(s.shape[4:], jnp.float32) for s in grads],
        in_specs=[pl.BlockSpec(memory_space=pl.ANY)] * n,
        out_specs=[pl.BlockSpec(memory_space=pltpu.VMEM)] * n,
        scratch_shapes=scratch
        + [
            pltpu.SemaphoreType.DMA((count,)),
            pltpu.SemaphoreType.DMA((count, 4, most)),
            pltpu.SemaphoreType.DMA((count, 4, most)),
        ],
        compiler_params=pltpu.CompilerParams(
            collective_id=collective_id, has_side_effects=True, vmem_limit_bytes=48 * 2**20
        ),
        name="scatter_grads",
    )(*grads)


HEADS = 12
HEAD_DIM = 64
LANDMARKS = 64
KERNEL = 33
NEWTON = 6
RIM = 16
FEATURES = HEADS * HEAD_DIM


highest_precision = lax.Precision.HIGHEST


def with_halo(x, sides, width):
    for axis, dim in sides:
        size, length = (lax.axis_size(axis), x.shape[dim])
        up = [(i, (i + 1) % size) for i in range(size - 1)]
        down = [(j, i) for i, j in up]
        last = lax.slice_in_dim(x, length - width, length, axis=dim)
        initial = lax.slice_in_dim(x, 0, width, axis=dim)
        before = lax.ppermute(last, axis, up)
        after = lax.ppermute(initial, axis, down)
        x = jnp.concatenate([before, x, after], axis=dim)
    return x


def merged(value, axis, join):
    pieces = jax.tree.map(lambda part: lax.all_gather(part, axis), value)
    head = jax.tree.map(lambda part: part[0], pieces)
    tail = jax.tree.map(lambda part: part[1:], pieces)
    subtotal, _ = lax.scan(lambda subtotal, piece: (join(subtotal, piece), None), head, tail)
    return subtotal


def for_sending(x):
    return jax.tree.map(lambda a: a.astype(jnp.bfloat16) if a.dtype == jnp.float32 else a, x)


def shifted(block, axis, distance):
    devices = range(lax.axis_size(axis))
    route = [(i - distance, i) for i in devices if i - distance in devices]
    return lax.ppermute(block, axis, route)


def layer_norm(rows, gain, shift):
    centre = rows - jnp.mean(rows, axis=-1, keepdims=True)
    spread = jnp.mean(centre * centre, axis=-1, keepdims=True)
    return centre * lax.rsqrt(spread + 1e-05) * gain + shift


def split_heads(matrix):
    return matrix.reshape(matrix.shape[:-1] + (HEADS, HEAD_DIM))


def pseudo_inverse(landmark_kernel_matrix):
    column_top = jnp.max(jnp.sum(landmark_kernel_matrix, axis=-2), axis=-1)
    row_top = jnp.max(jnp.sum(landmark_kernel_matrix, axis=-1), axis=-1)
    approx = jnp.swapaxes(landmark_kernel_matrix, -1, -2) / (column_top * row_top)[..., None, None]
    ident = jnp.eye(landmark_kernel_matrix.shape[-1], dtype=jnp.float32)
    for turn_index in range(NEWTON):
        product = jnp.matmul(landmark_kernel_matrix, approx, precision=highest_precision)
        inner = 7.0 * ident - product
        inner = 15.0 * ident - jnp.matmul(product, inner, precision=highest_precision)
        inner = 13.0 * ident - jnp.matmul(product, inner, precision=highest_precision)
        approx = 0.25 * jnp.matmul(approx, inner, precision=highest_precision)
    return approx


def landmark_mix(mark_query, mark_key, distant_values):
    scale = HEAD_DIM ** (-0.25)
    scores = jnp.einsum(
        "smhd,snhd->shmn",
        split_heads(mark_query) * scale,
        split_heads(mark_key) * scale,
        precision=highest_precision,
    )
    landmark_kernel_matrix = jax.nn.softmax(scores, axis=-1)
    inverse = pseudo_inverse(landmark_kernel_matrix)
    mixing_result = jnp.matmul(inverse, distant_values, precision=highest_precision)
    ident = jnp.eye(landmark_kernel_matrix.shape[-1], dtype=jnp.float32)
    defect = ident - jnp.matmul(landmark_kernel_matrix, inverse, precision=highest_precision)
    error = jnp.sum(jnp.sqrt(jnp.sum(defect * defect, axis=(-2, -1))))
    return (mixing_result, error)


def near_mix(queries, mark_key, mixing_result, value_ext, taps):
    scale = HEAD_DIM ** (-0.25)
    scores = jnp.einsum(
        "sthd,smhd->shtm",
        split_heads(queries) * scale,
        split_heads(mark_key) * scale,
        precision=highest_precision,
    )
    nearby_part = jax.nn.softmax(scores, axis=-1)
    attended_output = jnp.einsum(
        "shtm,shmd->sthd", nearby_part, mixing_result, precision=highest_precision
    )
    window = split_heads(value_ext)
    length = queries.shape[1]
    for tap_index in range(KERNEL):
        attended_output = (
            attended_output
            + taps[:, tap_index][:, None] * window[:, tap_index : tap_index + length]
        )
    return attended_output.reshape(queries.shape)


def far_scores(mark_query, key_rows):
    scale = HEAD_DIM ** (-0.25)
    return jnp.einsum(
        "smhd,sthd->shmt",
        split_heads(mark_query) * scale,
        split_heads(key_rows) * scale,
        precision=highest_precision,
    )


def far_stats(mark_query, key_rows, value_rows):
    scores = far_scores(mark_query, key_rows)
    peak = jnp.max(scores, axis=-1)
    expo = jnp.exp(scores - peak[..., None])
    total = jnp.sum(expo, axis=-1)
    numer = jnp.einsum(
        "shmt,sthd->shmd", expo, split_heads(value_rows), precision=highest_precision
    )
    return (peak, total, numer)


def far_change(mark_query, key_rows, value_rows, peak, total, distant_values):
    expo = jnp.exp(far_scores(mark_query, key_rows) - peak[..., None])
    numer = jnp.einsum(
        "shmt,sthd->shmd", expo, split_heads(value_rows), precision=highest_precision
    )
    return (numer - distant_values * jnp.sum(expo, axis=-1)[..., None]) / total[..., None]


def combine_stats(first, second):
    peak = jnp.maximum(first[0], second[0])
    first_weight = jnp.exp(first[0] - peak)
    second_weight = jnp.exp(second[0] - peak)
    total = first[1] * first_weight + second[1] * second_weight
    numer = first[2] * first_weight[..., None] + second[2] * second_weight[..., None]
    return (peak, total, numer)


def big_product(left, right):
    return jnp.einsum("std,de->ste", left, right, preferred_element_type=jnp.float32)


def weight_grad(left, right):
    return jnp.einsum("std,ste->de", left, right, preferred_element_type=jnp.float32)


def back_product(delta, weight):
    return jnp.einsum("ste,de->std", delta, weight, preferred_element_type=jnp.float32)


def bias_sum(delta):
    return jnp.sum(delta.astype(jnp.float32), axis=(0, 1))


def comm_parts(rows, wide):
    width = FEATURES
    parts = [(at, ALL, ALL) for at in range(4)]
    parts += [(4, ALL, slice(at * width, (at + 1) * width)) for at in range(wide)]
    parts += [(5, slice(at * rows, (at + 1) * rows), ALL) for at in range(wide)]
    return parts + [(6, ALL, ALL)]


def local(
    layer_input,
    query_weight,
    key_weight,
    value_weight,
    output_weight,
    up_weight,
    down_weight,
    query_bias,
    value_bias,
    output_bias,
    up_bias,
    down_bias,
    first_gain,
    first_shift,
    second_gain,
    second_shift,
    mixing_taps,
    output_cotangent,
):
    (
        full_query,
        full_key,
        full_value,
        full_output,
        full_up,
        full_down,
        bias_query,
        bias_value,
        bias_output,
        bias_up,
        bias_down,
        gain_first,
        shift_first,
        gain_second,
        shift_second,
    ) = (
        lax.all_gather(query_weight, BOTH, axis=0, tiled=True),
        lax.all_gather(key_weight, BOTH, axis=0, tiled=True),
        lax.all_gather(value_weight, BOTH, axis=0, tiled=True),
        lax.all_gather(output_weight, BOTH, axis=0, tiled=True),
        lax.all_gather(up_weight, BOTH, axis=0, tiled=True),
        lax.all_gather(down_weight, BOTH, axis=0, tiled=True),
        lax.all_gather(query_bias, BOTH, axis=0, tiled=True),
        lax.all_gather(value_bias, BOTH, axis=0, tiled=True),
        lax.all_gather(output_bias, BOTH, axis=0, tiled=True),
        lax.all_gather(up_bias, BOTH, axis=0, tiled=True),
        lax.all_gather(down_bias, BOTH, axis=0, tiled=True),
        lax.all_gather(first_gain, BOTH, axis=0, tiled=True),
        lax.all_gather(first_shift, BOTH, axis=0, tiled=True),
        lax.all_gather(second_gain, BOTH, axis=0, tiled=True),
        lax.all_gather(second_shift, BOTH, axis=0, tiled=True),
    )
    local_marks = LANDMARKS // lax.axis_size(SEQ)
    batch_rows, tokens, features = layer_input.shape
    segment = tokens // local_marks
    queries = big_product(layer_input, full_query) + bias_query.astype(jnp.float32)
    key_rows = big_product(layer_input, full_key)
    value_rows = (big_product(layer_input, full_value) + bias_value.astype(jnp.float32)).astype(
        jnp.bfloat16
    )
    mark_query = jnp.mean(
        queries.reshape(batch_rows, local_marks, segment, features), axis=2
    ).astype(jnp.bfloat16)
    mark_key = jnp.mean(
        key_rows.reshape(batch_rows, local_marks, segment, features), axis=2
    ).astype(jnp.bfloat16)
    all_query, all_key = (
        lax.all_gather(mark_query, SEQ, axis=1, tiled=True),
        lax.all_gather(mark_key, SEQ, axis=1, tiled=True),
    )
    value_ext = with_halo(value_rows, ((SEQ, 1),), RIM)
    query_marks = all_query.astype(jnp.float32)
    key_marks = all_key.astype(jnp.float32)
    value_float = value_rows.astype(jnp.float32)
    ext_float = value_ext.astype(jnp.float32)
    taps = mixing_taps.astype(jnp.float32)
    stat_peak, stat_total, stat_numer = far_stats(query_marks, key_rows, value_float)
    peak, total, numer = merged((stat_peak, stat_total, stat_numer), SEQ, combine_stats)
    distant_values = numer / total[..., None]
    mixing_result, mix_back, error = jax.vjp(
        landmark_mix, query_marks, key_marks, distant_values, has_aux=True
    )
    attended_output, near_back = jax.vjp(
        near_mix, queries, key_marks, mixing_result, ext_float, taps
    )
    attention = attended_output.astype(jnp.bfloat16)
    resid_first = (
        layer_input.astype(jnp.float32)
        + big_product(attention, full_output)
        + bias_output.astype(jnp.float32)
    )
    hidden, first_back = jax.vjp(
        layer_norm, resid_first, gain_first.astype(jnp.float32), shift_first.astype(jnp.float32)
    )
    hidden_low = hidden.astype(jnp.bfloat16)
    upper = big_product(hidden_low, full_up) + bias_up.astype(jnp.float32)
    activated, gelu_back = jax.vjp(partial(jax.nn.gelu, approximate=False), upper)
    activated_low = activated.astype(jnp.bfloat16)
    resid_second = hidden + big_product(activated_low, full_down) + bias_down.astype(jnp.float32)
    normed, second_back = jax.vjp(
        layer_norm, resid_second, gain_second.astype(jnp.float32), shift_second.astype(jnp.float32)
    )
    layer_output = normed.astype(jnp.bfloat16)
    pinv_error = lax.psum(error, BATCH) / (batch_rows * lax.axis_size(BATCH) * HEADS)
    delta_second, second_gain_grad, second_shift_grad = second_back(
        output_cotangent.astype(jnp.float32)
    )
    delta_lower = delta_second.astype(jnp.bfloat16)
    down_grad = weight_grad(activated_low, delta_lower)
    down_bias_grad = bias_sum(delta_lower)
    delta_upper = gelu_back(back_product(delta_lower, full_down))[0].astype(jnp.bfloat16)
    up_grad = weight_grad(hidden_low, delta_upper)
    up_bias_grad = bias_sum(delta_upper)
    delta_hidden = back_product(delta_upper, full_up) + delta_second
    delta_first, first_gain_grad, first_shift_grad = first_back(delta_hidden)
    delta_proj = delta_first.astype(jnp.bfloat16)
    output_grad = weight_grad(attention, delta_proj)
    output_bias_grad = bias_sum(delta_proj)
    delta_attention = back_product(delta_proj, full_output)
    delta_queries, key_part, mixing_part, delta_ext, taps_part = near_back(delta_attention)
    delta_mixing = jax.tree.map(
        lambda part: part.astype(jnp.float32), lax.psum(for_sending(mixing_part), SEQ)
    )
    query_rep, key_rep, delta_far = mix_back(delta_mixing)
    far_back = jax.vjp(
        partial(far_change, peak=peak, total=total, distant_values=distant_values),
        query_marks,
        key_rows,
        value_float,
    )[1]
    far_query, far_keys, far_vals = far_back(delta_far)
    own_key, own_query = (
        lax.psum_scatter(
            key_part.astype(jnp.bfloat16), SEQ, scatter_dimension=1, tiled=True
        ).astype(jnp.float32),
        lax.psum_scatter(
            far_query.astype(jnp.bfloat16), SEQ, scatter_dimension=1, tiled=True
        ).astype(jnp.float32),
    )
    start = lax.axis_index(SEQ) * local_marks
    own_query = own_query + lax.dynamic_slice_in_dim(query_rep, start, local_marks, 1)
    own_key = own_key + lax.dynamic_slice_in_dim(key_rep, start, local_marks, 1)

    def spread_marks(marks):
        shaped = jnp.broadcast_to(
            (marks / segment)[:, :, None, :], (batch_rows, local_marks, segment, features)
        )
        return shaped.reshape(batch_rows, tokens, features)

    query_delta = (delta_queries + spread_marks(own_query)).astype(jnp.bfloat16)
    key_delta = (far_keys + spread_marks(own_key)).astype(jnp.bfloat16)
    from_left = shifted(for_sending(delta_ext[:, :RIM]), SEQ, -1)
    from_right = shifted(for_sending(delta_ext[:, tokens + RIM :]), SEQ, 1)
    value_sum = delta_ext[:, RIM : RIM + tokens] + far_vals
    value_sum = value_sum + jnp.pad(from_left, ((0, 0), (tokens - RIM, 0), (0, 0)))
    value_sum = value_sum + jnp.pad(from_right, ((0, 0), (0, tokens - RIM), (0, 0)))
    value_delta = value_sum.astype(jnp.bfloat16)
    query_grad = weight_grad(layer_input, query_delta)
    key_grad = weight_grad(layer_input, key_delta)
    value_grad = weight_grad(layer_input, value_delta)
    query_bias_grad = bias_sum(query_delta)
    value_bias_grad = bias_sum(value_delta)
    input_gradient = (
        back_product(query_delta, full_query)
        + back_product(key_delta, full_key)
        + back_product(value_delta, full_value)
        + delta_first
    )
    taps_gradient = lax.psum(taps_part, BOTH)
    owned = (
        lax.psum_scatter(query_grad, BOTH, scatter_dimension=0, tiled=True),
        lax.psum_scatter(key_grad, BOTH, scatter_dimension=0, tiled=True),
        lax.psum_scatter(value_grad, BOTH, scatter_dimension=0, tiled=True),
        lax.psum_scatter(output_grad, BOTH, scatter_dimension=0, tiled=True),
        lax.psum_scatter(up_grad, BOTH, scatter_dimension=0, tiled=True),
        lax.psum_scatter(down_grad, BOTH, scatter_dimension=0, tiled=True),
        lax.psum_scatter(query_bias_grad, BOTH, scatter_dimension=0, tiled=True),
        lax.psum_scatter(value_bias_grad, BOTH, scatter_dimension=0, tiled=True),
        lax.psum_scatter(output_bias_grad, BOTH, scatter_dimension=0, tiled=True),
        lax.psum_scatter(up_bias_grad, BOTH, scatter_dimension=0, tiled=True),
        lax.psum_scatter(down_bias_grad, BOTH, scatter_dimension=0, tiled=True),
        lax.psum_scatter(first_gain_grad, BOTH, scatter_dimension=0, tiled=True),
        lax.psum_scatter(first_shift_grad, BOTH, scatter_dimension=0, tiled=True),
        lax.psum_scatter(second_gain_grad, BOTH, scatter_dimension=0, tiled=True),
        lax.psum_scatter(second_shift_grad, BOTH, scatter_dimension=0, tiled=True),
    )
    return (
        layer_output,
        input_gradient,
        owned[0],
        owned[1],
        owned[2],
        owned[3],
        owned[4],
        owned[5],
        owned[6],
        owned[7],
        owned[8],
        owned[9],
        owned[10],
        owned[11],
        owned[12],
        owned[13],
        owned[14],
        taps_gradient,
        pinv_error,
    )


def exchange_kernel(ways, *refs):
    n = len(ways)
    ins, outs = refs[:n], refs[n : 2 * n]
    send_sem, recv_sem = refs[2 * n :]
    size = lax.axis_size(SEQ)
    batch, me = lax.axis_index(BATCH), lax.axis_index(SEQ)
    barrier = pltpu.get_barrier_semaphore()

    def greet(step, carry):
        peer = lax.rem(me + step, size)
        pl.semaphore_signal(barrier, inc=1, device_id=(batch, peer), device_id_type=MESH)
        return carry

    lax.fori_loop(1, size, greet, 0)
    pl.semaphore_wait(barrier, size - 1)

    def copy_of(at, step):
        peer = lax.rem(me + step, size)
        source = ins[at].at[peer] if ways[at] == SCATTER else ins[at]
        target = outs[at].at[me] if ways[at] in (GATHER, SCATTER) else outs[at]
        return pltpu.make_async_remote_copy(
            src_ref=source,
            dst_ref=target,
            send_sem=send_sem.at[at, step],
            recv_sem=recv_sem.at[at, step],
            device_id=(batch, peer),
            device_id_type=MESH,
        )

    def start(step, carry):
        for at, way in enumerate(ways):
            if way in (GATHER, SCATTER):
                copy_of(at, step).start()
        return carry

    def finish(step, carry):
        for at, way in enumerate(ways):
            if way in (GATHER, SCATTER):
                copy_of(at, step).wait()
        return carry

    single = [(at, {NEXT: 1, LAST: size - 1}[way]) for at, way in enumerate(ways) if way in (NEXT, LAST)]
    for at, step in single:
        copy_of(at, step).start()
    lax.fori_loop(1, size, start, 0)
    for at, way in enumerate(ways):
        if way == GATHER:
            outs[at][me] = ins[at][...]
        elif way == SCATTER:
            outs[at][me] = ins[at][me]
    for at, step in single:
        copy_of(at, step).wait()
    lax.fori_loop(1, size, finish, 0)


def exchange(size, collective_id, *items):
    ways = tuple(way for way, _ in items)
    arrays = [array for _, array in items]
    shapes = [((size,) + a.shape if way == GATHER else a.shape) for way, a in items]
    vmem = pl.BlockSpec(memory_space=pltpu.VMEM)
    return pl.pallas_call(
        partial(exchange_kernel, ways),
        out_shape=[jax.ShapeDtypeStruct(shape, a.dtype) for shape, a in zip(shapes, arrays)],
        in_specs=[vmem] * len(ways),
        out_specs=[vmem] * len(ways),
        scratch_shapes=[
            pltpu.SemaphoreType.DMA((len(ways), size)),
            pltpu.SemaphoreType.DMA((len(ways), size)),
        ],
        compiler_params=pltpu.CompilerParams(collective_id=collective_id, has_side_effects=True),
        name="exchange",
    )(*arrays)


def own_mix(mark_query, mark_key, distant_values):
    scale = HEAD_DIM ** (-0.25)
    heads = distant_values.shape[0]

    def pair(marks):
        return marks.reshape(marks.shape[0], heads, HEAD_DIM) * scale

    scores = jnp.einsum("mhd,nhd->hmn", pair(mark_query), pair(mark_key), precision=highest_precision)
    landmark_kernel_matrix = jax.nn.softmax(scores, axis=-1)
    inverse = pseudo_inverse(landmark_kernel_matrix)
    mixing_result = jnp.matmul(inverse, distant_values, precision=highest_precision)
    ident = jnp.eye(landmark_kernel_matrix.shape[-1], dtype=jnp.float32)
    defect = ident - jnp.matmul(landmark_kernel_matrix, inverse, precision=highest_precision)
    error = jnp.sum(jnp.sqrt(jnp.sum(defect * defect, axis=(-2, -1))))
    return (mixing_result, error)


def far_back(mark_query, key_rows, value_rows, peak, total, delta_far, inner):
    scale = HEAD_DIM ** (-0.25)
    near_one = jnp.exp(far_scores(mark_query, key_rows) - peak[..., None]) / total[..., None]
    values = split_heads(value_rows)
    far_vals = jnp.einsum("shmt,shmd->sthd", near_one, delta_far, precision=highest_precision)
    slope = jnp.einsum("shmd,sthd->shmt", delta_far, values, precision=highest_precision)
    slope = near_one * (slope - inner[..., None])
    far_query = jnp.einsum("shmt,sthd->smhd", slope, split_heads(key_rows) * scale, precision=highest_precision)
    far_keys = jnp.einsum("shmt,smhd->sthd", slope, split_heads(mark_query) * scale, precision=highest_precision)
    return (
        (far_query * scale).reshape(mark_query.shape),
        (far_keys * scale).reshape(key_rows.shape),
        far_vals.reshape(value_rows.shape),
    )


def local_fast(
    batch,
    seq,
    layer_input,
    query_weight,
    key_weight,
    value_weight,
    output_weight,
    up_weight,
    down_weight,
    query_bias,
    value_bias,
    output_bias,
    up_bias,
    down_bias,
    first_gain,
    first_shift,
    second_gain,
    second_shift,
    mixing_taps,
    output_cotangent,
):
    weights = (query_weight, key_weight, value_weight, output_weight, up_weight, down_weight)
    vectors = (
        query_bias,
        value_bias,
        output_bias,
        down_bias,
        first_gain,
        first_shift,
        second_gain,
        second_shift,
    )
    own = query_bias.shape[0]
    wide = up_bias.shape[0] // own
    packed = jnp.concatenate([*(v[None] for v in vectors), up_bias.reshape(wide, own)], axis=0)
    packed = jnp.pad(packed, ((0, 16 - packed.shape[0]), (0, 128 - own)))
    parts = comm_parts(own, wide)
    orders = ["xy" if at % 2 == 0 else "yx" for at in range(len(parts))]
    *gathered, vectors_all = gather_weights(
        batch, seq, weights + (packed,), parts, orders, 2, 1
    )
    full_query, full_key, full_value, full_output, full_up, full_down = (
        whole.reshape(-1, whole.shape[-1]) for whole in gathered
    )
    table = jnp.swapaxes(vectors_all.reshape(batch * seq, 16, 128)[:, :, :own], 0, 1)
    (
        bias_query,
        bias_value,
        bias_output,
        bias_down,
        gain_first,
        shift_first,
        gain_second,
        shift_second,
    ) = (table[at].reshape(-1) for at in range(8))
    bias_up = jnp.swapaxes(table[8 : 8 + wide], 0, 1).reshape(-1)
    local_marks = LANDMARKS // lax.axis_size(SEQ)
    batch_rows, tokens, features = layer_input.shape
    segment = tokens // local_marks
    queries = big_product(layer_input, full_query) + bias_query.astype(jnp.float32)
    key_rows = big_product(layer_input, full_key)
    value_rows = (big_product(layer_input, full_value) + bias_value.astype(jnp.float32)).astype(
        jnp.bfloat16
    )
    mark_query = jnp.mean(
        queries.reshape(batch_rows, local_marks, segment, features), axis=2
    ).astype(jnp.bfloat16)
    mark_key = jnp.mean(
        key_rows.reshape(batch_rows, local_marks, segment, features), axis=2
    ).astype(jnp.bfloat16)
    marks, before, after = exchange(
        seq,
        3,
        (GATHER, jnp.stack([mark_query, mark_key])),
        (NEXT, value_rows[:, tokens - RIM :]),
        (LAST, value_rows[:, :RIM]),
    )
    place_at = lax.axis_index(SEQ)
    before = jnp.where(place_at > 0, before, jnp.zeros_like(before))
    after = jnp.where(place_at < seq - 1, after, jnp.zeros_like(after))
    value_ext = jnp.concatenate([before, value_rows, after], axis=1)
    marks = jnp.transpose(marks, (1, 2, 0, 3, 4)).reshape(2, batch_rows, LANDMARKS, features)
    query_marks, key_marks = marks[0].astype(jnp.float32), marks[1].astype(jnp.float32)
    value_float = value_rows.astype(jnp.float32)
    ext_float = value_ext.astype(jnp.float32)
    taps = mixing_taps.astype(jnp.float32)
    stat_peak, stat_total, stat_numer = far_stats(query_marks, key_rows, value_float)
    owners = batch_rows * HEADS // 2
    low = jnp.bfloat16

    def to_owners(matrices):
        pairs = matrices.reshape(owners, 2, LANDMARKS, HEAD_DIM).astype(low)
        pairs = jnp.swapaxes(pairs, 1, 2).reshape(owners, LANDMARKS, 2 * HEAD_DIM)
        return jnp.concatenate([pairs, pairs[: seq - owners]], axis=0)

    def as_pair(sides):
        return jnp.swapaxes(sides.reshape(LANDMARKS, 2, HEAD_DIM), 0, 1)

    def as_sides(pair):
        return jnp.swapaxes(pair, 0, 1).reshape(LANDMARKS, 2 * HEAD_DIM)

    def from_owners(sides):
        pairs = sides[:owners].reshape(owners, LANDMARKS, 2, HEAD_DIM).astype(jnp.float32)
        return jnp.swapaxes(pairs, 1, 2).reshape(batch_rows, HEADS, LANDMARKS, HEAD_DIM)

    def rows_to_owners(*rows):
        table = jnp.stack([row.reshape(owners, 2 * LANDMARKS) for row in rows], axis=1)
        table = jnp.pad(table, ((0, 0), (0, 8 - len(rows)), (0, 0)))
        return jnp.concatenate([table, table[: seq - owners]], axis=0)

    def rows_from_owners(table, at):
        return table[:owners, at].reshape(batch_rows, HEADS, LANDMARKS)

    numers, stats = exchange(
        seq,
        4,
        (SCATTER, to_owners(stat_numer)),
        (SCATTER, rows_to_owners(stat_peak, stat_total)),
    )
    peak_rows, total_rows = stats[:, 0], stats[:, 1]
    peak_own = jnp.max(peak_rows, axis=0)
    weights_own = jnp.exp(peak_rows - peak_own)
    total_own = jnp.sum(total_rows * weights_own, axis=0)
    numer_pairs = jnp.swapaxes(numers.astype(jnp.float32).reshape(seq, LANDMARKS, 2, HEAD_DIM), 1, 2)
    shares = (weights_own / total_own).reshape(seq, 2, LANDMARKS, 1)
    distant_own = jnp.sum(numer_pairs * shares, axis=0)
    owner = lax.rem(place_at, owners)
    own_row, own_lane = owner // (HEADS // 2), (owner % (HEADS // 2)) * 2 * HEAD_DIM

    def own_marks(all_marks):
        return lax.dynamic_slice(all_marks, (own_row, 0, own_lane), (1, LANDMARKS, 2 * HEAD_DIM))[0]

    mixing_own, mix_back, error = jax.vjp(
        own_mix, own_marks(query_marks), own_marks(key_marks), distant_own, has_aux=True
    )
    mixings, stats = exchange(
        seq,
        5,
        (GATHER, as_sides(mixing_own).astype(low)),
        (GATHER, jnp.pad(jnp.stack([peak_own, total_own]), ((0, 6), (0, 0)))),
    )
    mixing_result = from_owners(mixings)
    peak, total = rows_from_owners(stats, 0), rows_from_owners(stats, 1)
    attended_output, near_back = jax.vjp(
        near_mix, queries, key_marks, mixing_result, ext_float, taps
    )
    attention = attended_output.astype(jnp.bfloat16)
    resid_first = (
        layer_input.astype(jnp.float32)
        + big_product(attention, full_output)
        + bias_output.astype(jnp.float32)
    )
    hidden, first_back = jax.vjp(
        layer_norm, resid_first, gain_first.astype(jnp.float32), shift_first.astype(jnp.float32)
    )
    hidden_low = hidden.astype(jnp.bfloat16)
    upper = big_product(hidden_low, full_up) + bias_up.astype(jnp.float32)
    activated, gelu_back = jax.vjp(partial(jax.nn.gelu, approximate=False), upper)
    activated_low = activated.astype(jnp.bfloat16)
    resid_second = hidden + big_product(activated_low, full_down) + bias_down.astype(jnp.float32)
    normed, second_back = jax.vjp(
        layer_norm, resid_second, gain_second.astype(jnp.float32), shift_second.astype(jnp.float32)
    )
    layer_output = normed.astype(jnp.bfloat16)
    delta_second, second_gain_grad, second_shift_grad = second_back(
        output_cotangent.astype(jnp.float32)
    )
    delta_lower = delta_second.astype(jnp.bfloat16)
    down_grad = weight_grad(activated_low, delta_lower)
    down_bias_grad = bias_sum(delta_lower)
    delta_upper = gelu_back(back_product(delta_lower, full_down))[0].astype(jnp.bfloat16)
    up_grad = weight_grad(hidden_low, delta_upper)
    up_bias_grad = bias_sum(delta_upper)
    delta_hidden = back_product(delta_upper, full_up) + delta_second
    delta_first, first_gain_grad, first_shift_grad = first_back(delta_hidden)
    delta_proj = delta_first.astype(jnp.bfloat16)
    output_grad = weight_grad(attention, delta_proj)
    output_bias_grad = bias_sum(delta_proj)
    delta_attention = back_product(delta_proj, full_output)
    delta_queries, key_part, mixing_part, delta_ext, taps_part = near_back(delta_attention)
    (parts_own,) = exchange(seq, 6, (SCATTER, to_owners(mixing_part)))
    delta_mixing = as_pair(jnp.sum(parts_own.astype(jnp.float32), axis=0))
    query_own, key_own, far_own = mix_back(delta_mixing)
    inner_own = jnp.sum(far_own * distant_own, axis=-1).reshape(1, 2 * LANDMARKS)
    delta_fars, inners = exchange(
        seq,
        7,
        (GATHER, as_sides(far_own).astype(low)),
        (GATHER, jnp.pad(inner_own, ((0, 7), (0, 0)))),
    )
    far_query, far_keys, far_vals = far_back(
        query_marks, key_rows, value_float, peak, total, from_owners(delta_fars), rows_from_owners(inners, 0)
    )
    active = jnp.where(place_at < owners, 1.0, 0.0)

    def with_own(part, own):
        at = (own_row, 0, own_lane)
        held = lax.dynamic_slice(part, at, (1, LANDMARKS, 2 * HEAD_DIM))
        return lax.dynamic_update_slice(part, held + active * own[None], at)

    def by_owner(part):
        return jnp.swapaxes(part.reshape(batch_rows, seq, local_marks, features), 0, 1).astype(low)

    spread = jnp.stack(
        [by_owner(with_own(far_query, query_own)), by_owner(with_own(key_part, key_own))], axis=1
    )
    marks_parts, from_right, from_left = exchange(
        seq,
        8,
        (SCATTER, spread),
        (LAST, for_sending(delta_ext[:, :RIM])),
        (NEXT, for_sending(delta_ext[:, tokens + RIM :])),
    )
    from_right = jnp.where(place_at < seq - 1, from_right, jnp.zeros_like(from_right))
    from_left = jnp.where(place_at > 0, from_left, jnp.zeros_like(from_left))
    own_query, own_key = jnp.sum(marks_parts.astype(jnp.float32), axis=0)

    def spread_marks(marks):
        shaped = jnp.broadcast_to(
            (marks / segment)[:, :, None, :], (batch_rows, local_marks, segment, features)
        )
        return shaped.reshape(batch_rows, tokens, features)

    query_delta = (delta_queries + spread_marks(own_query)).astype(jnp.bfloat16)
    key_delta = (far_keys + spread_marks(own_key)).astype(jnp.bfloat16)
    value_sum = delta_ext[:, RIM : RIM + tokens] + far_vals
    value_sum = value_sum + jnp.pad(from_right, ((0, 0), (tokens - RIM, 0), (0, 0)))
    value_sum = value_sum + jnp.pad(from_left, ((0, 0), (0, tokens - RIM), (0, 0)))
    value_delta = value_sum.astype(jnp.bfloat16)
    query_grad = weight_grad(layer_input, query_delta)
    key_grad = weight_grad(layer_input, key_delta)
    value_grad = weight_grad(layer_input, value_delta)
    query_bias_grad = bias_sum(query_delta)
    value_bias_grad = bias_sum(value_delta)
    input_gradient = (
        back_product(query_delta, full_query)
        + back_product(key_delta, full_key)
        + back_product(value_delta, full_value)
        + delta_first
    )
    error_share = jnp.where(place_at < owners, error, 0.0) / (batch_rows * batch * HEADS)
    joined = jnp.concatenate([taps_part.reshape(-1), error_share[None]])
    joined = lax.psum(joined, BOTH)
    taps_gradient, pinv_error = joined[:-1].reshape(taps_part.shape), joined[-1]
    sizes = grid_of(batch, seq)
    grads = [
        grad.astype(jnp.bfloat16).reshape(sizes + (-1, grad.shape[-1]))
        for grad in (query_grad, key_grad, value_grad, output_grad, up_grad, down_grad)
    ]
    rows = [
        query_bias_grad,
        value_bias_grad,
        output_bias_grad,
        down_bias_grad,
        first_gain_grad,
        first_shift_grad,
        second_gain_grad,
        second_shift_grad,
    ]
    sums = jnp.concatenate(
        [
            jnp.swapaxes(jnp.stack(rows).reshape(8, batch * seq, own), 0, 1),
            up_bias_grad.reshape(batch * seq, wide, own),
        ],
        axis=1,
    )
    sums = jnp.pad(sums, ((0, 0), (0, 16 - sums.shape[1]), (0, 128 - own)))
    *owned, mine = scatter_grads(
        batch, seq, grads + [sums.reshape(sizes + (16, 128))], parts, orders, 2, 2
    )
    owned += [mine[0, :own], mine[1, :own], mine[2, :own], mine[8 : 8 + wide, :own].reshape(-1)]
    owned += [mine[at, :own] for at in range(3, 8)]
    return (
        layer_output,
        input_gradient,
        owned[0],
        owned[1],
        owned[2],
        owned[3],
        owned[4],
        owned[5],
        owned[6],
        owned[7],
        owned[8],
        owned[9],
        owned[10],
        owned[11],
        owned[12],
        owned[13],
        owned[14],
        taps_gradient,
        pinv_error,
    )


def solution(mesh):
    placed = (
        TOKENS,
        ROWS,
        ROWS,
        ROWS,
        ROWS,
        ROWS,
        ROWS,
        SPREAD,
        SPREAD,
        SPREAD,
        SPREAD,
        SPREAD,
        SPREAD,
        SPREAD,
        SPREAD,
        SPREAD,
        P(),
        TOKENS,
    )
    batch, seq = mesh.shape[BATCH], mesh.shape[SEQ]
    fits = seq == 16 and FEATURES % (8 * batch * seq) == 0
    return jax.shard_map(
        partial(local_fast, batch, seq) if fits else local,
        mesh=mesh,
        in_specs=placed,
        out_specs=(
            TOKENS,
            TOKENS,
            ROWS,
            ROWS,
            ROWS,
            ROWS,
            ROWS,
            ROWS,
            SPREAD,
            SPREAD,
            SPREAD,
            SPREAD,
            SPREAD,
            SPREAD,
            SPREAD,
            SPREAD,
            SPREAD,
            P(),
            P(),
        ),
        check_vma=False,
    )
```

```python
from functools import partial

import jax
import jax.numpy as jnp
from jax import lax
from jax.experimental import pallas as pl
from jax.experimental.pallas import tpu as pltpu
from jax.sharding import PartitionSpec as P

MESH = pl.DeviceIdType.MESH
BATCH, SEQ = "batch", "seq"
BOTH = (BATCH, SEQ)
ROWS, SPREAD, TOKENS = P(BOTH, None), P(BOTH), P(BATCH, SEQ, None)
GATHER, SCATTER, NEXT, LAST = range(4)
NEAR_SCORES, NEAR_OUT = "sthd,smhd->shtm", "shtm,shmd->sthd"
ALL = slice(None)
LAG = 1


def grid_of(batch, seq):
    mid = 2 if seq < 32 else 4
    return batch, seq // (2 * mid), mid, 2


class Grid:
    def __init__(self, batch, seq):
        self.sizes = dict(zip("xzyc", grid_of(batch, seq)))
        s = lax.axis_index(SEQ)
        ny, nc = self.sizes["y"], self.sizes["c"]
        self.at = {"x": lax.axis_index(BATCH), "z": s // (ny * nc), "y": (s // nc) % ny, "c": s % nc}

    def device(self, at):
        return (at["x"], (at["z"] * self.sizes["y"] + at["y"]) * self.sizes["c"] + at["c"])

    def others(self, axis):
        size = self.sizes[axis]
        return [(step, lax.rem(self.at[axis] + step, size)) for step in range(1, size)]

    def moved(self, axis, other):
        return self.device({**self.at, axis: other})

    def greet(self):
        barrier = pltpu.get_barrier_semaphore()
        count = 0
        for axis in "zxyc":
            for _, other in self.others(axis):
                pl.semaphore_signal(barrier, inc=1, device_id=self.moved(axis, other), device_id_type=MESH)
                count += 1
        pl.semaphore_wait(barrier, count)

    def block(self, whole):
        return tuple(ALL if axis in whole else self.at[axis] for axis in "xzyc")


def gather_kernel(batch, seq, parts, orders, unit, n_in, *refs):
    ins, outs = refs[:n_in], refs[n_in : 2 * n_in]
    send_sem, recv_sem, own_sem = refs[2 * n_in :]
    g = Grid(batch, seq)
    g.greet()
    count = len(parts)
    copies = {}

    def view(part, whole):
        index, rows, cols = parts[part]
        return outs[index].at[g.block(whole) + (rows, cols)]

    def send(part, stage, axis, source, target):
        started = []
        for step, other in g.others(axis):
            copy = pltpu.make_async_remote_copy(
                src_ref=source,
                dst_ref=target,
                send_sem=send_sem.at[part, stage, step - 1],
                recv_sem=recv_sem.at[part, stage, step - 1],
                device_id=g.moved(axis, other),
                device_id_type=MESH,
            )
            copy.start()
            started.append(copy)
        copies[part, stage] = started

    def arrive(part, stage):
        for copy in copies[part, stage]:
            copy.wait_recv()

    def begin(part):
        index, rows, cols = parts[part]
        source = ins[index].at[rows, cols]
        own = pltpu.make_async_copy(source, view(part, ""), own_sem.at[part])
        own.start()
        copies[part, "own"] = own
        send(part, 0, "z", source, view(part, ""))

    def spread(stage):
        def run(part):
            axes = ("z",) + tuple(orders[part]) + ("c",)
            if stage == 1:
                copies[part, "own"].wait()
            arrive(part, stage - 1)
            if stage < 4:
                held = view(part, axes[:stage])
                send(part, stage, axes[stage], held, held)
        return run

    units = [range(at, min(at + unit, count)) for at in range(0, count, unit)]
    stages = [begin] + [spread(stage) for stage in (1, 2, 3, 4)]
    for turn in range(len(units) + 4 * LAG):
        for lag, stage in enumerate(stages):
            if 0 <= turn - lag * LAG < len(units):
                for part in units[turn - lag * LAG]:
                    stage(part)
    for part in range(count):
        for stage in range(4):
            for copy in copies[part, stage]:
                copy.wait_send()


def gather_weights(batch, seq, shards, parts, orders, unit, collective_id):
    sizes = grid_of(batch, seq)
    n, count, most = len(shards), len(parts), max(sizes) - 1
    return pl.pallas_call(
        partial(gather_kernel, batch, seq, parts, orders, unit, n),
        out_shape=[jax.ShapeDtypeStruct(sizes + s.shape, s.dtype) for s in shards],
        in_specs=[pl.BlockSpec(memory_space=pltpu.VMEM)] * n,
        out_specs=[pl.BlockSpec(memory_space=pl.ANY)] * n,
        scratch_shapes=[
            pltpu.SemaphoreType.DMA((count, 4, most)),
            pltpu.SemaphoreType.DMA((count, 4, most)),
            pltpu.SemaphoreType.DMA((count,)),
        ],
        compiler_params=pltpu.CompilerParams(collective_id=collective_id, has_side_effects=True),
        name="gather_weights",
    )(*shards)


def scatter_kernel(batch, seq, parts, orders, unit, n_in, *refs):
    ins, outs = refs[:n_in], refs[n_in : 2 * n_in]
    own_sem, send_sem, recv_sem = refs[-3:]
    scratch = refs[2 * n_in : -3]
    g = Grid(batch, seq)
    g.greet()
    count = len(parts)
    copies = {}
    shapes = [part_shape(ins, part) for part in parts]
    groups = sorted(set(shapes), key=shapes.index)
    held, from_core, far, from_near, from_line = ([None] * count for _ in range(5))
    for at, shape in enumerate(groups):
        members = [part for part in range(count) if shapes[part] == shape]
        buffers = scratch[6 * at : 6 * at + 6]
        for rank, part in enumerate(members):
            far_rank = [p for p in members if orders[p] == orders[part]].index(part)
            held[part], from_core[part] = buffers[0].at[rank], buffers[1].at[rank]
            far[part] = (buffers[2] if orders[part][1] == "y" else buffers[3]).at[far_rank]
            from_near[part], from_line[part] = buffers[4].at[rank], buffers[5].at[rank]

    def source(part, core):
        index, rows, cols = parts[part]
        return ins[index].at[ALL, ALL, ALL, core, rows, cols]

    def mine(part, whole, **moved):
        at = {**g.at, **moved}
        return held[part].at[tuple(ALL if axis in whole else at[axis] for axis in "xzy")]

    def send(part, stage, axis, step, other, src, dst):
        copy = pltpu.make_async_remote_copy(
            src_ref=src,
            dst_ref=dst,
            send_sem=send_sem.at[part, stage, step - 1],
            recv_sem=recv_sem.at[part, stage, step - 1],
            device_id=g.moved(axis, other),
            device_id_type=MESH,
        )
        copy.start()
        copies.setdefault((part, stage), []).append(copy)

    def accumulate(into, others):
        lead = into.shape[:-2]
        total = 1
        for size in lead:
            total *= size

        def step(i, carry):
            at = []
            for size in reversed(lead):
                at.insert(0, i % size)
                i = i // size
            at = tuple(at)
            value = into[at].astype(jnp.float32)
            for other in others:
                value += other[at].astype(jnp.float32)
            into[at] = value.astype(into.dtype)
            return carry

        lax.fori_loop(0, total, step, 0)

    def begin(part):
        own = pltpu.make_async_copy(source(part, g.at["c"]), held[part], own_sem.at[part])
        own.start()
        copies[part, "own"] = own
        for step, other in g.others("c"):
            send(part, 0, "c", step, other, source(part, other), from_core[part])

    def arrive(part, stage):
        for copy in copies[part, stage]:
            copy.wait_recv()

    def reduce_core(part):
        copies[part, "own"].wait()
        arrive(part, 0)
        accumulate(held[part], [from_core[part]])
        axis = orders[part][1]
        whole = "xzy".replace(axis, "")
        for step, other in g.others(axis):
            send(part, 1, axis, step, other, mine(part, whole, **{axis: other}), far[part].at[step - 1])

    def reduce_far(part):
        arrive(part, 1)
        near, axis = orders[part]
        accumulate(
            mine(part, "xzy".replace(axis, "")), [far[part].at[step - 1] for step, _ in g.others(axis)]
        )
        for step, other in g.others(near):
            send(part, 2, near, step, other, mine(part, "z", **{near: other}), from_near[part].at[step - 1])

    def reduce_near(part):
        arrive(part, 2)
        near = orders[part][0]
        accumulate(mine(part, "z"), [from_near[part].at[step - 1] for step, _ in g.others(near)])
        for step, other in g.others("z"):
            send(part, 3, "z", step, other, mine(part, "", z=other), from_line[part].at[step - 1])

    def reduce_line(part):
        arrive(part, 3)
        index, rows, cols = parts[part]
        own, size = mine(part, "")[...].astype(jnp.float32), g.sizes["z"]
        value = None
        for z in range(size):
            step = lax.rem(g.at["z"] - z + size, size)
            came = from_line[part][lax.rem(step + size - 2, size - 1)].astype(jnp.float32)
            term = jnp.where(step == 0, own, came)
            value = term if value is None else value + term
        outs[index][rows, cols] = value

    units = [range(at, min(at + unit, count)) for at in range(0, count, unit)]
    stages = [begin, reduce_core, reduce_far, reduce_near, reduce_line]
    for turn in range(len(units) + 4 * LAG):
        for lag, stage in enumerate(stages):
            if 0 <= turn - lag * LAG < len(units):
                for part in units[turn - lag * LAG]:
                    stage(part)
    for part in range(count):
        for stage in range(4):
            for copy in copies[part, stage]:
                copy.wait_send()


def part_shape(arrays, part):
    index, rows, cols = part
    array = arrays[index]
    spans = [len(range(*span.indices(size))) for span, size in zip((rows, cols), array.shape[-2:])]
    return (*spans, array.dtype)


def scatter_grads(batch, seq, grads, parts, orders, unit, collective_id):
    sizes = nx, nz, ny, nc = grid_of(batch, seq)
    n, count, most = len(grads), len(parts), max(sizes) - 1
    shapes = [part_shape(grads, part) for part in parts]
    scratch = []
    for shape in sorted(set(shapes), key=shapes.index):
        members = [part for part in range(count) if shapes[part] == shape]
        rows, cols, kind = shape
        ways = [orders[part] for part in members]
        total = len(members)
        scratch += [
            pltpu.VMEM((total, nx, nz, ny, rows, cols), kind),
            pltpu.VMEM((total, nx, nz, ny, rows, cols), kind),
            pltpu.VMEM((max(1, ways.count("xy")), ny - 1, nx, nz, rows, cols), kind),
            pltpu.VMEM((max(1, ways.count("yx")), nx - 1, nz, ny, rows, cols), kind),
            pltpu.VMEM((total, max(nx, ny) - 1, nz, rows, cols), kind),
            pltpu.VMEM((total, nz - 1, rows, cols), kind),
        ]
    return pl.pallas_call(
        partial(scatter_kernel, batch, seq, parts, orders, unit, n),
        out_shape=[jax.ShapeDtypeStruct(s.shape[4:], jnp.float32) for s in grads],
        in_specs=[pl.BlockSpec(memory_space=pl.ANY)] * n,
        out_specs=[pl.BlockSpec(memory_space=pltpu.VMEM)] * n,
        scratch_shapes=scratch
        + [
            pltpu.SemaphoreType.DMA((count,)),
            pltpu.SemaphoreType.DMA((count, 4, most)),
            pltpu.SemaphoreType.DMA((count, 4, most)),
        ],
        compiler_params=pltpu.CompilerParams(
            collective_id=collective_id, has_side_effects=True, vmem_limit_bytes=48 * 2**20
        ),
        name="scatter_grads",
    )(*grads)


HEADS = 12
HEAD_DIM = 64
LANDMARKS = 64
KERNEL = 33
NEWTON = 6
RIM = 16
FEATURES = HEADS * HEAD_DIM


highest_precision = lax.Precision.HIGHEST


def with_halo(x, sides, width):
    for axis, dim in sides:
        size, length = (lax.axis_size(axis), x.shape[dim])
        up = [(i, (i + 1) % size) for i in range(size - 1)]
        down = [(j, i) for i, j in up]
        last = lax.slice_in_dim(x, length - width, length, axis=dim)
        initial = lax.slice_in_dim(x, 0, width, axis=dim)
        before = lax.ppermute(last, axis, up)
        after = lax.ppermute(initial, axis, down)
        x = jnp.concatenate([before, x, after], axis=dim)
    return x


def merged(value, axis, join):
    pieces = jax.tree.map(lambda part: lax.all_gather(part, axis), value)
    head = jax.tree.map(lambda part: part[0], pieces)
    tail = jax.tree.map(lambda part: part[1:], pieces)
    subtotal, _ = lax.scan(lambda subtotal, piece: (join(subtotal, piece), None), head, tail)
    return subtotal


def for_sending(x):
    return jax.tree.map(lambda a: a.astype(jnp.bfloat16) if a.dtype == jnp.float32 else a, x)


def shifted(block, axis, distance):
    devices = range(lax.axis_size(axis))
    route = [(i - distance, i) for i in devices if i - distance in devices]
    return lax.ppermute(block, axis, route)


def layer_norm(rows, gain, shift):
    centre = rows - jnp.mean(rows, axis=-1, keepdims=True)
    spread = jnp.mean(centre * centre, axis=-1, keepdims=True)
    return centre * lax.rsqrt(spread + 1e-05) * gain + shift


def split_heads(matrix):
    return matrix.reshape(matrix.shape[:-1] + (HEADS, HEAD_DIM))


def pseudo_inverse(landmark_kernel_matrix):
    column_top = jnp.max(jnp.sum(landmark_kernel_matrix, axis=-2), axis=-1)
    row_top = jnp.max(jnp.sum(landmark_kernel_matrix, axis=-1), axis=-1)
    approx = jnp.swapaxes(landmark_kernel_matrix, -1, -2) / (column_top * row_top)[..., None, None]
    ident = jnp.eye(landmark_kernel_matrix.shape[-1], dtype=jnp.float32)
    for turn_index in range(NEWTON):
        product = jnp.matmul(landmark_kernel_matrix, approx, precision=highest_precision)
        inner = 7.0 * ident - product
        inner = 15.0 * ident - jnp.matmul(product, inner, precision=highest_precision)
        inner = 13.0 * ident - jnp.matmul(product, inner, precision=highest_precision)
        approx = 0.25 * jnp.matmul(approx, inner, precision=highest_precision)
    return approx


def landmark_mix(mark_query, mark_key, distant_values):
    scale = HEAD_DIM ** (-0.25)
    scores = jnp.einsum(
        "smhd,snhd->shmn",
        split_heads(mark_query) * scale,
        split_heads(mark_key) * scale,
        precision=highest_precision,
    )
    landmark_kernel_matrix = jax.nn.softmax(scores, axis=-1)
    inverse = pseudo_inverse(landmark_kernel_matrix)
    mixing_result = jnp.matmul(inverse, distant_values, precision=highest_precision)
    ident = jnp.eye(landmark_kernel_matrix.shape[-1], dtype=jnp.float32)
    defect = ident - jnp.matmul(landmark_kernel_matrix, inverse, precision=highest_precision)
    error = jnp.sum(jnp.sqrt(jnp.sum(defect * defect, axis=(-2, -1))))
    return (mixing_result, error)


def near_mix(queries, mark_key, mixing_result, value_ext, taps):
    scale = HEAD_DIM ** (-0.25)
    scores = jnp.einsum(
        NEAR_SCORES,
        split_heads(queries) * scale,
        split_heads(mark_key) * scale,
        precision=highest_precision,
    )
    nearby_part = jax.nn.softmax(scores, axis=-1)
    attended_output = jnp.einsum(
        NEAR_OUT, nearby_part, mixing_result, precision=highest_precision
    )
    window = split_heads(value_ext)
    length = queries.shape[1]
    for tap_index in range(KERNEL):
        attended_output = (
            attended_output
            + taps[:, tap_index][:, None] * window[:, tap_index : tap_index + length]
        )
    return attended_output.reshape(queries.shape)


def far_scores(mark_query, key_rows):
    scale = HEAD_DIM ** (-0.25)
    return jnp.einsum(
        "smhd,sthd->shmt",
        split_heads(mark_query) * scale,
        split_heads(key_rows) * scale,
        precision=highest_precision,
    )


def far_stats(mark_query, key_rows, value_rows):
    scores = far_scores(mark_query, key_rows)
    peak = jnp.max(scores, axis=-1)
    expo = jnp.exp(scores - peak[..., None])
    total = jnp.sum(expo, axis=-1)
    numer = jnp.einsum(
        "shmt,sthd->shmd", expo, split_heads(value_rows), precision=highest_precision
    )
    return (peak, total, numer)


def far_change(mark_query, key_rows, value_rows, peak, total, distant_values):
    expo = jnp.exp(far_scores(mark_query, key_rows) - peak[..., None])
    numer = jnp.einsum(
        "shmt,sthd->shmd", expo, split_heads(value_rows), precision=highest_precision
    )
    return (numer - distant_values * jnp.sum(expo, axis=-1)[..., None]) / total[..., None]


def combine_stats(first, second):
    peak = jnp.maximum(first[0], second[0])
    first_weight = jnp.exp(first[0] - peak)
    second_weight = jnp.exp(second[0] - peak)
    total = first[1] * first_weight + second[1] * second_weight
    numer = first[2] * first_weight[..., None] + second[2] * second_weight[..., None]
    return (peak, total, numer)


def big_product(left, right):
    return jnp.einsum("std,de->ste", left, right, preferred_element_type=jnp.float32)


def weight_grad(left, right):
    return jnp.einsum("std,ste->de", left, right, preferred_element_type=jnp.float32)


def back_product(delta, weight):
    return jnp.einsum("ste,de->std", delta, weight, preferred_element_type=jnp.float32)


def bias_sum(delta):
    return jnp.sum(delta.astype(jnp.float32), axis=(0, 1))


def comm_parts(rows, wide):
    width = FEATURES
    parts = [(at, ALL, ALL) for at in range(4)]
    parts += [(4, ALL, slice(at * width, (at + 1) * width)) for at in range(wide)]
    parts += [(5, slice(at * rows, (at + 1) * rows), ALL) for at in range(wide)]
    return parts + [(6, ALL, ALL)]


def local(
    layer_input,
    query_weight,
    key_weight,
    value_weight,
    output_weight,
    up_weight,
    down_weight,
    query_bias,
    value_bias,
    output_bias,
    up_bias,
    down_bias,
    first_gain,
    first_shift,
    second_gain,
    second_shift,
    mixing_taps,
    output_cotangent,
):
    (
        full_query,
        full_key,
        full_value,
        full_output,
        full_up,
        full_down,
        bias_query,
        bias_value,
        bias_output,
        bias_up,
        bias_down,
        gain_first,
        shift_first,
        gain_second,
        shift_second,
    ) = (
        lax.all_gather(query_weight, BOTH, axis=0, tiled=True),
        lax.all_gather(key_weight, BOTH, axis=0, tiled=True),
        lax.all_gather(value_weight, BOTH, axis=0, tiled=True),
        lax.all_gather(output_weight, BOTH, axis=0, tiled=True),
        lax.all_gather(up_weight, BOTH, axis=0, tiled=True),
        lax.all_gather(down_weight, BOTH, axis=0, tiled=True),
        lax.all_gather(query_bias, BOTH, axis=0, tiled=True),
        lax.all_gather(value_bias, BOTH, axis=0, tiled=True),
        lax.all_gather(output_bias, BOTH, axis=0, tiled=True),
        lax.all_gather(up_bias, BOTH, axis=0, tiled=True),
        lax.all_gather(down_bias, BOTH, axis=0, tiled=True),
        lax.all_gather(first_gain, BOTH, axis=0, tiled=True),
        lax.all_gather(first_shift, BOTH, axis=0, tiled=True),
        lax.all_gather(second_gain, BOTH, axis=0, tiled=True),
        lax.all_gather(second_shift, BOTH, axis=0, tiled=True),
    )
    local_marks = LANDMARKS // lax.axis_size(SEQ)
    batch_rows, tokens, features = layer_input.shape
    segment = tokens // local_marks
    queries = big_product(layer_input, full_query) + bias_query.astype(jnp.float32)
    key_rows = big_product(layer_input, full_key)
    value_rows = (big_product(layer_input, full_value) + bias_value.astype(jnp.float32)).astype(
        jnp.bfloat16
    )
    mark_query = jnp.mean(
        queries.reshape(batch_rows, local_marks, segment, features), axis=2
    ).astype(jnp.bfloat16)
    mark_key = jnp.mean(
        key_rows.reshape(batch_rows, local_marks, segment, features), axis=2
    ).astype(jnp.bfloat16)
    all_query, all_key = (
        lax.all_gather(mark_query, SEQ, axis=1, tiled=True),
        lax.all_gather(mark_key, SEQ, axis=1, tiled=True),
    )
    value_ext = with_halo(value_rows, ((SEQ, 1),), RIM)
    query_marks = all_query.astype(jnp.float32)
    key_marks = all_key.astype(jnp.float32)
    value_float = value_rows.astype(jnp.float32)
    ext_float = value_ext.astype(jnp.float32)
    taps = mixing_taps.astype(jnp.float32)
    stat_peak, stat_total, stat_numer = far_stats(query_marks, key_rows, value_float)
    peak, total, numer = merged((stat_peak, stat_total, stat_numer), SEQ, combine_stats)
    distant_values = numer / total[..., None]
    mixing_result, mix_back, error = jax.vjp(
        landmark_mix, query_marks, key_marks, distant_values, has_aux=True
    )
    attended_output, near_back = jax.vjp(
        near_mix, queries, key_marks, mixing_result, ext_float, taps
    )
    attention = attended_output.astype(jnp.bfloat16)
    resid_first = (
        layer_input.astype(jnp.float32)
        + big_product(attention, full_output)
        + bias_output.astype(jnp.float32)
    )
    hidden, first_back = jax.vjp(
        layer_norm, resid_first, gain_first.astype(jnp.float32), shift_first.astype(jnp.float32)
    )
    hidden_low = hidden.astype(jnp.bfloat16)
    upper = big_product(hidden_low, full_up) + bias_up.astype(jnp.float32)
    activated, gelu_back = jax.vjp(partial(jax.nn.gelu, approximate=False), upper)
    activated_low = activated.astype(jnp.bfloat16)
    resid_second = hidden + big_product(activated_low, full_down) + bias_down.astype(jnp.float32)
    normed, second_back = jax.vjp(
        layer_norm, resid_second, gain_second.astype(jnp.float32), shift_second.astype(jnp.float32)
    )
    layer_output = normed.astype(jnp.bfloat16)
    pinv_error = lax.psum(error, BATCH) / (batch_rows * lax.axis_size(BATCH) * HEADS)
    delta_second, second_gain_grad, second_shift_grad = second_back(
        output_cotangent.astype(jnp.float32)
    )
    delta_lower = delta_second.astype(jnp.bfloat16)
    down_grad = weight_grad(activated_low, delta_lower)
    down_bias_grad = bias_sum(delta_lower)
    delta_upper = gelu_back(back_product(delta_lower, full_down))[0].astype(jnp.bfloat16)
    up_grad = weight_grad(hidden_low, delta_upper)
    up_bias_grad = bias_sum(delta_upper)
    delta_hidden = back_product(delta_upper, full_up) + delta_second
    delta_first, first_gain_grad, first_shift_grad = first_back(delta_hidden)
    delta_proj = delta_first.astype(jnp.bfloat16)
    output_grad = weight_grad(attention, delta_proj)
    output_bias_grad = bias_sum(delta_proj)
    delta_attention = back_product(delta_proj, full_output)
    delta_queries, key_part, mixing_part, delta_ext, taps_part = near_back(delta_attention)
    delta_mixing = jax.tree.map(
        lambda part: part.astype(jnp.float32), lax.psum(for_sending(mixing_part), SEQ)
    )
    query_rep, key_rep, delta_far = mix_back(delta_mixing)
    far_back = jax.vjp(
        partial(far_change, peak=peak, total=total, distant_values=distant_values),
        query_marks,
        key_rows,
        value_float,
    )[1]
    far_query, far_keys, far_vals = far_back(delta_far)
    own_key, own_query = (
        lax.psum_scatter(
            key_part.astype(jnp.bfloat16), SEQ, scatter_dimension=1, tiled=True
        ).astype(jnp.float32),
        lax.psum_scatter(
            far_query.astype(jnp.bfloat16), SEQ, scatter_dimension=1, tiled=True
        ).astype(jnp.float32),
    )
    start = lax.axis_index(SEQ) * local_marks
    own_query = own_query + lax.dynamic_slice_in_dim(query_rep, start, local_marks, 1)
    own_key = own_key + lax.dynamic_slice_in_dim(key_rep, start, local_marks, 1)

    def spread_marks(marks):
        shaped = jnp.broadcast_to(
            (marks / segment)[:, :, None, :], (batch_rows, local_marks, segment, features)
        )
        return shaped.reshape(batch_rows, tokens, features)

    query_delta = (delta_queries + spread_marks(own_query)).astype(jnp.bfloat16)
    key_delta = (far_keys + spread_marks(own_key)).astype(jnp.bfloat16)
    from_left = shifted(for_sending(delta_ext[:, :RIM]), SEQ, -1)
    from_right = shifted(for_sending(delta_ext[:, tokens + RIM :]), SEQ, 1)
    value_sum = delta_ext[:, RIM : RIM + tokens] + far_vals
    value_sum = value_sum + jnp.pad(from_left, ((0, 0), (tokens - RIM, 0), (0, 0)))
    value_sum = value_sum + jnp.pad(from_right, ((0, 0), (0, tokens - RIM), (0, 0)))
    value_delta = value_sum.astype(jnp.bfloat16)
    query_grad = weight_grad(layer_input, query_delta)
    key_grad = weight_grad(layer_input, key_delta)
    value_grad = weight_grad(layer_input, value_delta)
    query_bias_grad = bias_sum(query_delta)
    value_bias_grad = bias_sum(value_delta)
    input_gradient = (
        back_product(query_delta, full_query)
        + back_product(key_delta, full_key)
        + back_product(value_delta, full_value)
        + delta_first
    )
    taps_gradient = lax.psum(taps_part, BOTH)
    owned = (
        lax.psum_scatter(query_grad, BOTH, scatter_dimension=0, tiled=True),
        lax.psum_scatter(key_grad, BOTH, scatter_dimension=0, tiled=True),
        lax.psum_scatter(value_grad, BOTH, scatter_dimension=0, tiled=True),
        lax.psum_scatter(output_grad, BOTH, scatter_dimension=0, tiled=True),
        lax.psum_scatter(up_grad, BOTH, scatter_dimension=0, tiled=True),
        lax.psum_scatter(down_grad, BOTH, scatter_dimension=0, tiled=True),
        lax.psum_scatter(query_bias_grad, BOTH, scatter_dimension=0, tiled=True),
        lax.psum_scatter(value_bias_grad, BOTH, scatter_dimension=0, tiled=True),
        lax.psum_scatter(output_bias_grad, BOTH, scatter_dimension=0, tiled=True),
        lax.psum_scatter(up_bias_grad, BOTH, scatter_dimension=0, tiled=True),
        lax.psum_scatter(down_bias_grad, BOTH, scatter_dimension=0, tiled=True),
        lax.psum_scatter(first_gain_grad, BOTH, scatter_dimension=0, tiled=True),
        lax.psum_scatter(first_shift_grad, BOTH, scatter_dimension=0, tiled=True),
        lax.psum_scatter(second_gain_grad, BOTH, scatter_dimension=0, tiled=True),
        lax.psum_scatter(second_shift_grad, BOTH, scatter_dimension=0, tiled=True),
    )
    return (
        layer_output,
        input_gradient,
        owned[0],
        owned[1],
        owned[2],
        owned[3],
        owned[4],
        owned[5],
        owned[6],
        owned[7],
        owned[8],
        owned[9],
        owned[10],
        owned[11],
        owned[12],
        owned[13],
        owned[14],
        taps_gradient,
        pinv_error,
    )


def exchange_kernel(ways, *refs):
    n = len(ways)
    ins, outs = refs[:n], refs[n : 2 * n]
    send_sem, recv_sem = refs[2 * n :]
    size = lax.axis_size(SEQ)
    batch, me = lax.axis_index(BATCH), lax.axis_index(SEQ)
    barrier = pltpu.get_barrier_semaphore()

    def greet(step, carry):
        peer = lax.rem(me + step, size)
        pl.semaphore_signal(barrier, inc=1, device_id=(batch, peer), device_id_type=MESH)
        return carry

    lax.fori_loop(1, size, greet, 0)
    pl.semaphore_wait(barrier, size - 1)

    def copy_of(at, step):
        peer = lax.rem(me + step, size)
        source = ins[at].at[peer] if ways[at] == SCATTER else ins[at]
        target = outs[at].at[me] if ways[at] in (GATHER, SCATTER) else outs[at]
        return pltpu.make_async_remote_copy(
            src_ref=source,
            dst_ref=target,
            send_sem=send_sem.at[at, step],
            recv_sem=recv_sem.at[at, step],
            device_id=(batch, peer),
            device_id_type=MESH,
        )

    def start(step, carry):
        for at, way in enumerate(ways):
            if way in (GATHER, SCATTER):
                copy_of(at, step).start()
        return carry

    def finish(step, carry):
        for at, way in enumerate(ways):
            if way in (GATHER, SCATTER):
                copy_of(at, step).wait()
        return carry

    single = [(at, {NEXT: 1, LAST: size - 1}[way]) for at, way in enumerate(ways) if way in (NEXT, LAST)]
    for at, step in single:
        copy_of(at, step).start()
    lax.fori_loop(1, size, start, 0)
    for at, way in enumerate(ways):
        if way == GATHER:
            outs[at][me] = ins[at][...]
        elif way == SCATTER:
            outs[at][me] = ins[at][me]
    for at, step in single:
        copy_of(at, step).wait()
    lax.fori_loop(1, size, finish, 0)


def exchange(size, collective_id, *items):
    ways = tuple(way for way, _ in items)
    arrays = [array for _, array in items]
    shapes = [((size,) + a.shape if way == GATHER else a.shape) for way, a in items]
    vmem = pl.BlockSpec(memory_space=pltpu.VMEM)
    return pl.pallas_call(
        partial(exchange_kernel, ways),
        out_shape=[jax.ShapeDtypeStruct(shape, a.dtype) for shape, a in zip(shapes, arrays)],
        in_specs=[vmem] * len(ways),
        out_specs=[vmem] * len(ways),
        scratch_shapes=[
            pltpu.SemaphoreType.DMA((len(ways), size)),
            pltpu.SemaphoreType.DMA((len(ways), size)),
        ],
        compiler_params=pltpu.CompilerParams(collective_id=collective_id, has_side_effects=True),
        name="exchange",
    )(*arrays)


def own_mix(mark_query, mark_key, distant_values):
    scale = HEAD_DIM ** (-0.25)
    heads = distant_values.shape[0]

    def pair(marks):
        return marks.reshape(marks.shape[0], heads, HEAD_DIM) * scale

    scores = jnp.einsum("mhd,nhd->hmn", pair(mark_query), pair(mark_key), precision=highest_precision)
    landmark_kernel_matrix = jax.nn.softmax(scores, axis=-1)
    inverse = pseudo_inverse(landmark_kernel_matrix)
    mixing_result = jnp.matmul(inverse, distant_values, precision=highest_precision)
    ident = jnp.eye(landmark_kernel_matrix.shape[-1], dtype=jnp.float32)
    defect = ident - jnp.matmul(landmark_kernel_matrix, inverse, precision=highest_precision)
    error = jnp.sum(jnp.sqrt(jnp.sum(defect * defect, axis=(-2, -1))))
    return (mixing_result, error)


def far_back(mark_query, key_rows, value_rows, peak, total, delta_far, inner):
    scale = HEAD_DIM ** (-0.25)
    near_one = jnp.exp(far_scores(mark_query, key_rows) - peak[..., None]) / total[..., None]
    values = split_heads(value_rows)
    far_vals = jnp.einsum("shmt,shmd->sthd", near_one, delta_far, precision=highest_precision)
    slope = jnp.einsum("shmd,sthd->shmt", delta_far, values, precision=highest_precision)
    slope = near_one * (slope - inner[..., None])
    far_query = jnp.einsum("shmt,sthd->smhd", slope, split_heads(key_rows) * scale, precision=highest_precision)
    far_keys = jnp.einsum("shmt,smhd->sthd", slope, split_heads(mark_query) * scale, precision=highest_precision)
    return (
        (far_query * scale).reshape(mark_query.shape),
        (far_keys * scale).reshape(key_rows.shape),
        far_vals.reshape(value_rows.shape),
    )


def near_mix_banded(queries, mark_key, mixing_result, value_ext, taps):
    scale = HEAD_DIM ** (-0.25)
    scores = jnp.einsum(
        NEAR_SCORES, split_heads(queries) * scale, split_heads(mark_key) * scale, precision=highest_precision
    )
    nearby_part = jax.nn.softmax(scores, axis=-1)
    attended_output = jnp.einsum(NEAR_OUT, nearby_part, mixing_result, precision=highest_precision)
    length, reach = queries.shape[1], value_ext.shape[1]
    shape = (KERNEL, length, reach)
    tap, token, source = (lax.broadcasted_iota(jnp.int32, shape, at) for at in range(3))
    chosen = (source - token == tap).astype(jnp.float32)
    banded = jnp.einsum("hj,jtu->htu", taps, chosen, precision=highest_precision)
    attended_output = attended_output + jnp.einsum(
        "htu,suhd->sthd", banded, split_heads(value_ext), precision=highest_precision
    )
    return attended_output.reshape(queries.shape)


def local_fast(
    batch,
    seq,
    layer_input,
    query_weight,
    key_weight,
    value_weight,
    output_weight,
    up_weight,
    down_weight,
    query_bias,
    value_bias,
    output_bias,
    up_bias,
    down_bias,
    first_gain,
    first_shift,
    second_gain,
    second_shift,
    mixing_taps,
    output_cotangent,
):
    weights = (query_weight, key_weight, value_weight, output_weight, up_weight, down_weight)
    vectors = (
        query_bias,
        value_bias,
        output_bias,
        down_bias,
        first_gain,
        first_shift,
        second_gain,
        second_shift,
    )
    own = query_bias.shape[0]
    wide = up_bias.shape[0] // own
    packed = jnp.concatenate([*(v[None] for v in vectors), up_bias.reshape(wide, own)], axis=0)
    packed = jnp.pad(packed, ((0, 16 - packed.shape[0]), (0, 128 - own)))
    parts = comm_parts(own, wide)
    orders = ["xy" if at % 2 == 0 else "yx" for at in range(len(parts))]
    *gathered, vectors_all = gather_weights(
        batch, seq, weights + (packed,), parts, orders, 2, 1
    )
    full_query, full_key, full_value, full_output, full_up, full_down = (
        whole.reshape(-1, whole.shape[-1]) for whole in gathered
    )
    table = jnp.swapaxes(vectors_all.reshape(batch * seq, 16, 128)[:, :, :own], 0, 1)
    (
        bias_query,
        bias_value,
        bias_output,
        bias_down,
        gain_first,
        shift_first,
        gain_second,
        shift_second,
    ) = (table[at].reshape(-1) for at in range(8))
    bias_up = jnp.swapaxes(table[8 : 8 + wide], 0, 1).reshape(-1)
    local_marks = LANDMARKS // lax.axis_size(SEQ)
    batch_rows, tokens, features = layer_input.shape
    segment = tokens // local_marks
    queries = big_product(layer_input, full_query) + bias_query.astype(jnp.float32)
    key_rows = big_product(layer_input, full_key)
    value_rows = (big_product(layer_input, full_value) + bias_value.astype(jnp.float32)).astype(
        jnp.bfloat16
    )
    mark_query = jnp.mean(
        queries.reshape(batch_rows, local_marks, segment, features), axis=2
    ).astype(jnp.bfloat16)
    mark_key = jnp.mean(
        key_rows.reshape(batch_rows, local_marks, segment, features), axis=2
    ).astype(jnp.bfloat16)
    marks, before, after = exchange(
        seq,
        3,
        (GATHER, jnp.stack([mark_query, mark_key])),
        (NEXT, value_rows[:, tokens - RIM :]),
        (LAST, value_rows[:, :RIM]),
    )
    place_at = lax.axis_index(SEQ)
    before = jnp.where(place_at > 0, before, jnp.zeros_like(before))
    after = jnp.where(place_at < seq - 1, after, jnp.zeros_like(after))
    value_ext = jnp.concatenate([before, value_rows, after], axis=1)
    marks = jnp.transpose(marks, (1, 2, 0, 3, 4)).reshape(2, batch_rows, LANDMARKS, features)
    query_marks, key_marks = marks[0].astype(jnp.float32), marks[1].astype(jnp.float32)
    value_float = value_rows.astype(jnp.float32)
    ext_float = value_ext.astype(jnp.float32)
    taps = mixing_taps.astype(jnp.float32)
    stat_peak, stat_total, stat_numer = far_stats(query_marks, key_rows, value_float)
    owners = batch_rows * HEADS // 2
    low = jnp.bfloat16

    def to_owners(matrices):
        pairs = matrices.reshape(owners, 2, LANDMARKS, HEAD_DIM).astype(low)
        pairs = jnp.swapaxes(pairs, 1, 2).reshape(owners, LANDMARKS, 2 * HEAD_DIM)
        return jnp.concatenate([pairs, pairs[: seq - owners]], axis=0)

    def as_pair(sides):
        return jnp.swapaxes(sides.reshape(LANDMARKS, 2, HEAD_DIM), 0, 1)

    def as_sides(pair):
        return jnp.swapaxes(pair, 0, 1).reshape(LANDMARKS, 2 * HEAD_DIM)

    def from_owners(sides):
        pairs = sides[:owners].reshape(owners, LANDMARKS, 2, HEAD_DIM).astype(jnp.float32)
        return jnp.swapaxes(pairs, 1, 2).reshape(batch_rows, HEADS, LANDMARKS, HEAD_DIM)

    def rows_to_owners(*rows):
        table = jnp.stack([row.reshape(owners, 2 * LANDMARKS) for row in rows], axis=1)
        table = jnp.pad(table, ((0, 0), (0, 8 - len(rows)), (0, 0)))
        return jnp.concatenate([table, table[: seq - owners]], axis=0)

    def rows_from_owners(table, at):
        return table[:owners, at].reshape(batch_rows, HEADS, LANDMARKS)

    numers, stats = exchange(
        seq,
        4,
        (SCATTER, to_owners(stat_numer)),
        (SCATTER, rows_to_owners(stat_peak, stat_total)),
    )
    peak_rows, total_rows = stats[:, 0], stats[:, 1]
    peak_own = jnp.max(peak_rows, axis=0)
    weights_own = jnp.exp(peak_rows - peak_own)
    total_own = jnp.sum(total_rows * weights_own, axis=0)
    numer_pairs = jnp.swapaxes(numers.astype(jnp.float32).reshape(seq, LANDMARKS, 2, HEAD_DIM), 1, 2)
    shares = (weights_own / total_own).reshape(seq, 2, LANDMARKS, 1)
    distant_own = jnp.sum(numer_pairs * shares, axis=0)
    owner = lax.rem(place_at, owners)
    own_row, own_lane = owner // (HEADS // 2), (owner % (HEADS // 2)) * 2 * HEAD_DIM

    def own_marks(all_marks):
        return lax.dynamic_slice(all_marks, (own_row, 0, own_lane), (1, LANDMARKS, 2 * HEAD_DIM))[0]

    mixing_own, mix_back, error = jax.vjp(
        own_mix, own_marks(query_marks), own_marks(key_marks), distant_own, has_aux=True
    )
    mixings, stats = exchange(
        seq,
        5,
        (GATHER, as_sides(mixing_own).astype(low)),
        (GATHER, jnp.pad(jnp.stack([peak_own, total_own]), ((0, 6), (0, 0)))),
    )
    mixing_result = from_owners(mixings)
    peak, total = rows_from_owners(stats, 0), rows_from_owners(stats, 1)
    attended_output, near_back = jax.vjp(
        near_mix_banded, queries, key_marks, mixing_result, ext_float, taps
    )
    attention = attended_output.astype(jnp.bfloat16)
    resid_first = (
        layer_input.astype(jnp.float32)
        + big_product(attention, full_output)
        + bias_output.astype(jnp.float32)
    )
    hidden, first_back = jax.vjp(
        layer_norm, resid_first, gain_first.astype(jnp.float32), shift_first.astype(jnp.float32)
    )
    hidden_low = hidden.astype(jnp.bfloat16)
    upper = big_product(hidden_low, full_up) + bias_up.astype(jnp.float32)
    activated, gelu_back = jax.vjp(partial(jax.nn.gelu, approximate=False), upper)
    activated_low = activated.astype(jnp.bfloat16)
    resid_second = hidden + big_product(activated_low, full_down) + bias_down.astype(jnp.float32)
    normed, second_back = jax.vjp(
        layer_norm, resid_second, gain_second.astype(jnp.float32), shift_second.astype(jnp.float32)
    )
    layer_output = normed.astype(jnp.bfloat16)
    delta_second, second_gain_grad, second_shift_grad = second_back(
        output_cotangent.astype(jnp.float32)
    )
    delta_lower = delta_second.astype(jnp.bfloat16)
    down_grad = weight_grad(activated_low, delta_lower)
    down_bias_grad = bias_sum(delta_lower)
    delta_upper = gelu_back(back_product(delta_lower, full_down))[0].astype(jnp.bfloat16)
    up_grad = weight_grad(hidden_low, delta_upper)
    up_bias_grad = bias_sum(delta_upper)
    delta_hidden = back_product(delta_upper, full_up) + delta_second
    delta_first, first_gain_grad, first_shift_grad = first_back(delta_hidden)
    delta_proj = delta_first.astype(jnp.bfloat16)
    output_grad = weight_grad(attention, delta_proj)
    output_bias_grad = bias_sum(delta_proj)
    delta_attention = back_product(delta_proj, full_output)
    delta_queries, key_part, mixing_part, delta_ext, taps_part = near_back(delta_attention)
    (parts_own,) = exchange(seq, 6, (SCATTER, to_owners(mixing_part)))
    delta_mixing = as_pair(jnp.sum(parts_own.astype(jnp.float32), axis=0))
    query_own, key_own, far_own = mix_back(delta_mixing)
    inner_own = jnp.sum(far_own * distant_own, axis=-1).reshape(1, 2 * LANDMARKS)
    delta_fars, inners = exchange(
        seq,
        7,
        (GATHER, as_sides(far_own).astype(low)),
        (GATHER, jnp.pad(inner_own, ((0, 7), (0, 0)))),
    )
    far_query, far_keys, far_vals = far_back(
        query_marks, key_rows, value_float, peak, total, from_owners(delta_fars), rows_from_owners(inners, 0)
    )
    active = jnp.where(place_at < owners, 1.0, 0.0)

    def with_own(part, own):
        at = (own_row, 0, own_lane)
        held = lax.dynamic_slice(part, at, (1, LANDMARKS, 2 * HEAD_DIM))
        return lax.dynamic_update_slice(part, held + active * own[None], at)

    def by_owner(part):
        return jnp.swapaxes(part.reshape(batch_rows, seq, local_marks, features), 0, 1).astype(low)

    spread = jnp.stack(
        [by_owner(with_own(far_query, query_own)), by_owner(with_own(key_part, key_own))], axis=1
    )
    marks_parts, from_right, from_left = exchange(
        seq,
        8,
        (SCATTER, spread),
        (LAST, for_sending(delta_ext[:, :RIM])),
        (NEXT, for_sending(delta_ext[:, tokens + RIM :])),
    )
    from_right = jnp.where(place_at < seq - 1, from_right, jnp.zeros_like(from_right))
    from_left = jnp.where(place_at > 0, from_left, jnp.zeros_like(from_left))
    own_query, own_key = jnp.sum(marks_parts.astype(jnp.float32), axis=0)

    def spread_marks(marks):
        shaped = jnp.broadcast_to(
            (marks / segment)[:, :, None, :], (batch_rows, local_marks, segment, features)
        )
        return shaped.reshape(batch_rows, tokens, features)

    query_delta = (delta_queries + spread_marks(own_query)).astype(jnp.bfloat16)
    key_delta = (far_keys + spread_marks(own_key)).astype(jnp.bfloat16)
    value_sum = delta_ext[:, RIM : RIM + tokens] + far_vals
    value_sum = value_sum + jnp.pad(from_right, ((0, 0), (tokens - RIM, 0), (0, 0)))
    value_sum = value_sum + jnp.pad(from_left, ((0, 0), (0, tokens - RIM), (0, 0)))
    value_delta = value_sum.astype(jnp.bfloat16)
    query_grad = weight_grad(layer_input, query_delta)
    key_grad = weight_grad(layer_input, key_delta)
    value_grad = weight_grad(layer_input, value_delta)
    query_bias_grad = bias_sum(query_delta)
    value_bias_grad = bias_sum(value_delta)
    input_gradient = (
        back_product(query_delta, full_query)
        + back_product(key_delta, full_key)
        + back_product(value_delta, full_value)
        + delta_first
    )
    error_share = jnp.where(place_at < owners, error, 0.0) / (batch_rows * batch * HEADS)
    joined = jnp.concatenate([taps_part.reshape(-1), error_share[None]])
    joined = jnp.pad(joined, (0, 4 * 128 - joined.shape[0])).reshape(1, 4, 128)
    sizes = grid_of(batch, seq)
    grads = [
        grad.astype(jnp.bfloat16).reshape(sizes + (-1, grad.shape[-1]))
        for grad in (query_grad, key_grad, value_grad, output_grad, up_grad, down_grad)
    ]
    rows = [
        query_bias_grad,
        value_bias_grad,
        output_bias_grad,
        down_bias_grad,
        first_gain_grad,
        first_shift_grad,
        second_gain_grad,
        second_shift_grad,
    ]
    sums = jnp.concatenate(
        [
            jnp.swapaxes(jnp.stack(rows).reshape(8, batch * seq, own), 0, 1),
            up_bias_grad.reshape(batch * seq, wide, own),
        ],
        axis=1,
    )
    sums = jnp.pad(sums, ((0, 0), (0, 0), (0, 128 - own)))
    sums = jnp.concatenate([sums, jnp.broadcast_to(joined, (batch * seq, 4, 128))], axis=1)
    *owned, mine = scatter_grads(
        batch, seq, grads + [sums.reshape(sizes + (16, 128))], parts, orders, 2, 2
    )
    joined = mine[12:].reshape(-1)
    taps_gradient = joined[: HEADS * KERNEL].reshape(taps_part.shape)
    pinv_error = joined[HEADS * KERNEL]
    owned += [mine[0, :own], mine[1, :own], mine[2, :own], mine[8 : 8 + wide, :own].reshape(-1)]
    owned += [mine[at, :own] for at in range(3, 8)]
    return (
        layer_output,
        input_gradient,
        owned[0],
        owned[1],
        owned[2],
        owned[3],
        owned[4],
        owned[5],
        owned[6],
        owned[7],
        owned[8],
        owned[9],
        owned[10],
        owned[11],
        owned[12],
        owned[13],
        owned[14],
        taps_gradient,
        pinv_error,
    )


def solution(mesh):
    placed = (
        TOKENS,
        ROWS,
        ROWS,
        ROWS,
        ROWS,
        ROWS,
        ROWS,
        SPREAD,
        SPREAD,
        SPREAD,
        SPREAD,
        SPREAD,
        SPREAD,
        SPREAD,
        SPREAD,
        SPREAD,
        P(),
        TOKENS,
    )
    batch, seq = mesh.shape[BATCH], mesh.shape[SEQ]
    fits = seq == 16 and FEATURES % (8 * batch * seq) == 0
    return jax.shard_map(
        partial(local_fast, batch, seq) if fits else local,
        mesh=mesh,
        in_specs=placed,
        out_specs=(
            TOKENS,
            TOKENS,
            ROWS,
            ROWS,
            ROWS,
            ROWS,
            ROWS,
            ROWS,
            SPREAD,
            SPREAD,
            SPREAD,
            SPREAD,
            SPREAD,
            SPREAD,
            SPREAD,
            SPREAD,
            SPREAD,
            P(),
            P(),
        ),
        check_vma=False,
    )
```

```python
from functools import partial

import jax
import jax.numpy as jnp
from jax import lax
from jax.experimental import pallas as pl
from jax.experimental.pallas import tpu as pltpu
from jax.sharding import PartitionSpec as P

MESH = pl.DeviceIdType.MESH
BATCH, SEQ = "batch", "seq"
BOTH = (BATCH, SEQ)
ROWS, SPREAD, TOKENS = P(BOTH, None), P(BOTH), P(BATCH, SEQ, None)
GATHER, SCATTER, NEXT, LAST, SUM = range(5)
NEAR_SCORES, NEAR_OUT = "sthd,smhd->shtm", "shtm,shmd->sthd"
ALL = slice(None)
LAG = 1


def grid_of(batch, seq):
    mid = 2 if seq < 32 else 4
    return batch, seq // (2 * mid), mid, 2


class Grid:
    def __init__(self, batch, seq):
        self.sizes = dict(zip("xzyc", grid_of(batch, seq)))
        s = lax.axis_index(SEQ)
        ny, nc = self.sizes["y"], self.sizes["c"]
        self.at = {"x": lax.axis_index(BATCH), "z": s // (ny * nc), "y": (s // nc) % ny, "c": s % nc}

    def device(self, at):
        return (at["x"], (at["z"] * self.sizes["y"] + at["y"]) * self.sizes["c"] + at["c"])

    def others(self, axis):
        size = self.sizes[axis]
        return [(step, lax.rem(self.at[axis] + step, size)) for step in range(1, size)]

    def moved(self, axis, other):
        return self.device({**self.at, axis: other})

    def greet(self):
        barrier = pltpu.get_barrier_semaphore()
        count = 0
        for axis in "zxyc":
            for _, other in self.others(axis):
                pl.semaphore_signal(barrier, inc=1, device_id=self.moved(axis, other), device_id_type=MESH)
                count += 1
        pl.semaphore_wait(barrier, count)

    def block(self, whole):
        return tuple(ALL if axis in whole else self.at[axis] for axis in "xzyc")


def gather_kernel(batch, seq, parts, orders, unit, n_in, *refs):
    ins, outs = refs[:n_in], refs[n_in : 2 * n_in]
    send_sem, recv_sem, own_sem = refs[2 * n_in :]
    g = Grid(batch, seq)
    g.greet()
    count = len(parts)
    copies = {}

    def view(part, whole):
        index, rows, cols = parts[part]
        return outs[index].at[g.block(whole) + (rows, cols)]

    def send(part, stage, axis, source, target):
        started = []
        for step, other in g.others(axis):
            copy = pltpu.make_async_remote_copy(
                src_ref=source,
                dst_ref=target,
                send_sem=send_sem.at[part, stage, step - 1],
                recv_sem=recv_sem.at[part, stage, step - 1],
                device_id=g.moved(axis, other),
                device_id_type=MESH,
            )
            copy.start()
            started.append(copy)
        copies[part, stage] = started

    def arrive(part, stage):
        for copy in copies[part, stage]:
            copy.wait_recv()

    def begin(part):
        index, rows, cols = parts[part]
        source = ins[index].at[rows, cols]
        own = pltpu.make_async_copy(source, view(part, ""), own_sem.at[part])
        own.start()
        copies[part, "own"] = own
        send(part, 0, "z", source, view(part, ""))

    def spread(stage):
        def run(part):
            axes = ("z",) + tuple(orders[part]) + ("c",)
            if stage == 1:
                copies[part, "own"].wait()
            arrive(part, stage - 1)
            if stage < 4:
                held = view(part, axes[:stage])
                send(part, stage, axes[stage], held, held)
        return run

    units = [range(at, min(at + unit, count)) for at in range(0, count, unit)]
    stages = [begin] + [spread(stage) for stage in (1, 2, 3, 4)]
    for turn in range(len(units) + 4 * LAG):
        for lag, stage in enumerate(stages):
            if 0 <= turn - lag * LAG < len(units):
                for part in units[turn - lag * LAG]:
                    stage(part)
    for part in range(count):
        for stage in range(4):
            for copy in copies[part, stage]:
                copy.wait_send()


def gather_weights(batch, seq, shards, parts, orders, unit, collective_id):
    sizes = grid_of(batch, seq)
    n, count, most = len(shards), len(parts), max(sizes) - 1
    return pl.pallas_call(
        partial(gather_kernel, batch, seq, parts, orders, unit, n),
        out_shape=[jax.ShapeDtypeStruct(sizes + s.shape, s.dtype) for s in shards],
        in_specs=[pl.BlockSpec(memory_space=pltpu.VMEM)] * n,
        out_specs=[pl.BlockSpec(memory_space=pl.ANY)] * n,
        scratch_shapes=[
            pltpu.SemaphoreType.DMA((count, 4, most)),
            pltpu.SemaphoreType.DMA((count, 4, most)),
            pltpu.SemaphoreType.DMA((count,)),
        ],
        compiler_params=pltpu.CompilerParams(collective_id=collective_id, has_side_effects=True),
        name="gather_weights",
    )(*shards)


def scatter_kernel(batch, seq, parts, orders, unit, n_in, *refs):
    ins, outs = refs[:n_in], refs[n_in : 2 * n_in]
    own_sem, send_sem, recv_sem = refs[-3:]
    scratch = refs[2 * n_in : -3]
    g = Grid(batch, seq)
    g.greet()
    count = len(parts)
    copies = {}
    shapes = [part_shape(ins, part) for part in parts]
    groups = sorted(set(shapes), key=shapes.index)
    held, from_core, far, from_near, from_line = ([None] * count for _ in range(5))
    for at, shape in enumerate(groups):
        members = [part for part in range(count) if shapes[part] == shape]
        buffers = scratch[6 * at : 6 * at + 6]
        for rank, part in enumerate(members):
            far_rank = [p for p in members if orders[p] == orders[part]].index(part)
            held[part], from_core[part] = buffers[0].at[rank], buffers[1].at[rank]
            far[part] = (buffers[2] if orders[part][1] == "y" else buffers[3]).at[far_rank]
            from_near[part], from_line[part] = buffers[4].at[rank], buffers[5].at[rank]

    def source(part, core):
        index, rows, cols = parts[part]
        return ins[index].at[ALL, ALL, ALL, core, rows, cols]

    def mine(part, whole, **moved):
        at = {**g.at, **moved}
        return held[part].at[tuple(ALL if axis in whole else at[axis] for axis in "xzy")]

    def send(part, stage, axis, step, other, src, dst):
        copy = pltpu.make_async_remote_copy(
            src_ref=src,
            dst_ref=dst,
            send_sem=send_sem.at[part, stage, step - 1],
            recv_sem=recv_sem.at[part, stage, step - 1],
            device_id=g.moved(axis, other),
            device_id_type=MESH,
        )
        copy.start()
        copies.setdefault((part, stage), []).append(copy)

    def accumulate(into, others):
        lead = into.shape[:-2]
        total = 1
        for size in lead:
            total *= size

        def step(i, carry):
            at = []
            for size in reversed(lead):
                at.insert(0, i % size)
                i = i // size
            at = tuple(at)
            value = into[at].astype(jnp.float32)
            for other in others:
                value += other[at].astype(jnp.float32)
            into[at] = value.astype(into.dtype)
            return carry

        lax.fori_loop(0, total, step, 0)

    def begin(part):
        own = pltpu.make_async_copy(source(part, g.at["c"]), held[part], own_sem.at[part])
        own.start()
        copies[part, "own"] = own
        for step, other in g.others("c"):
            send(part, 0, "c", step, other, source(part, other), from_core[part])

    def arrive(part, stage):
        for copy in copies[part, stage]:
            copy.wait_recv()

    def reduce_core(part):
        copies[part, "own"].wait()
        arrive(part, 0)
        accumulate(held[part], [from_core[part]])
        axis = orders[part][1]
        whole = "xzy".replace(axis, "")
        for step, other in g.others(axis):
            send(part, 1, axis, step, other, mine(part, whole, **{axis: other}), far[part].at[step - 1])

    def reduce_far(part):
        arrive(part, 1)
        near, axis = orders[part]
        accumulate(
            mine(part, "xzy".replace(axis, "")), [far[part].at[step - 1] for step, _ in g.others(axis)]
        )
        for step, other in g.others(near):
            send(part, 2, near, step, other, mine(part, "z", **{near: other}), from_near[part].at[step - 1])

    def reduce_near(part):
        arrive(part, 2)
        near = orders[part][0]
        accumulate(mine(part, "z"), [from_near[part].at[step - 1] for step, _ in g.others(near)])
        for step, other in g.others("z"):
            send(part, 3, "z", step, other, mine(part, "", z=other), from_line[part].at[step - 1])

    def reduce_line(part):
        arrive(part, 3)
        index, rows, cols = parts[part]
        own, size = mine(part, "")[...].astype(jnp.float32), g.sizes["z"]
        value = None
        for z in range(size):
            step = lax.rem(g.at["z"] - z + size, size)
            came = from_line[part][lax.rem(step + size - 2, size - 1)].astype(jnp.float32)
            term = jnp.where(step == 0, own, came)
            value = term if value is None else value + term
        outs[index][rows, cols] = value

    units = [range(at, min(at + unit, count)) for at in range(0, count, unit)]
    stages = [begin, reduce_core, reduce_far, reduce_near, reduce_line]
    for turn in range(len(units) + 4 * LAG):
        for lag, stage in enumerate(stages):
            if 0 <= turn - lag * LAG < len(units):
                for part in units[turn - lag * LAG]:
                    stage(part)
    for part in range(count):
        for stage in range(4):
            for copy in copies[part, stage]:
                copy.wait_send()


def part_shape(arrays, part):
    index, rows, cols = part
    array = arrays[index]
    spans = [len(range(*span.indices(size))) for span, size in zip((rows, cols), array.shape[-2:])]
    return (*spans, array.dtype)


def scatter_grads(batch, seq, grads, parts, orders, unit, collective_id):
    sizes = nx, nz, ny, nc = grid_of(batch, seq)
    n, count, most = len(grads), len(parts), max(sizes) - 1
    shapes = [part_shape(grads, part) for part in parts]
    scratch = []
    for shape in sorted(set(shapes), key=shapes.index):
        members = [part for part in range(count) if shapes[part] == shape]
        rows, cols, kind = shape
        ways = [orders[part] for part in members]
        total = len(members)
        scratch += [
            pltpu.VMEM((total, nx, nz, ny, rows, cols), kind),
            pltpu.VMEM((total, nx, nz, ny, rows, cols), kind),
            pltpu.VMEM((max(1, ways.count("xy")), ny - 1, nx, nz, rows, cols), kind),
            pltpu.VMEM((max(1, ways.count("yx")), nx - 1, nz, ny, rows, cols), kind),
            pltpu.VMEM((total, max(nx, ny) - 1, nz, rows, cols), kind),
            pltpu.VMEM((total, nz - 1, rows, cols), kind),
        ]
    return pl.pallas_call(
        partial(scatter_kernel, batch, seq, parts, orders, unit, n),
        out_shape=[jax.ShapeDtypeStruct(s.shape[4:], jnp.float32) for s in grads],
        in_specs=[pl.BlockSpec(memory_space=pl.ANY)] * n,
        out_specs=[pl.BlockSpec(memory_space=pltpu.VMEM)] * n,
        scratch_shapes=scratch
        + [
            pltpu.SemaphoreType.DMA((count,)),
            pltpu.SemaphoreType.DMA((count, 4, most)),
            pltpu.SemaphoreType.DMA((count, 4, most)),
        ],
        compiler_params=pltpu.CompilerParams(
            collective_id=collective_id, has_side_effects=True, vmem_limit_bytes=48 * 2**20
        ),
        name="scatter_grads",
    )(*grads)


HEADS = 12
HEAD_DIM = 64
LANDMARKS = 64
KERNEL = 33
NEWTON = 6
RIM = 16
FEATURES = HEADS * HEAD_DIM


highest_precision = lax.Precision.HIGHEST


def with_halo(x, sides, width):
    for axis, dim in sides:
        size, length = (lax.axis_size(axis), x.shape[dim])
        up = [(i, (i + 1) % size) for i in range(size - 1)]
        down = [(j, i) for i, j in up]
        last = lax.slice_in_dim(x, length - width, length, axis=dim)
        initial = lax.slice_in_dim(x, 0, width, axis=dim)
        before = lax.ppermute(last, axis, up)
        after = lax.ppermute(initial, axis, down)
        x = jnp.concatenate([before, x, after], axis=dim)
    return x


def merged(value, axis, join):
    pieces = jax.tree.map(lambda part: lax.all_gather(part, axis), value)
    head = jax.tree.map(lambda part: part[0], pieces)
    tail = jax.tree.map(lambda part: part[1:], pieces)
    subtotal, _ = lax.scan(lambda subtotal, piece: (join(subtotal, piece), None), head, tail)
    return subtotal


def for_sending(x):
    return jax.tree.map(lambda a: a.astype(jnp.bfloat16) if a.dtype == jnp.float32 else a, x)


def shifted(block, axis, distance):
    devices = range(lax.axis_size(axis))
    route = [(i - distance, i) for i in devices if i - distance in devices]
    return lax.ppermute(block, axis, route)


def layer_norm(rows, gain, shift):
    centre = rows - jnp.mean(rows, axis=-1, keepdims=True)
    spread = jnp.mean(centre * centre, axis=-1, keepdims=True)
    return centre * lax.rsqrt(spread + 1e-05) * gain + shift


def split_heads(matrix):
    return matrix.reshape(matrix.shape[:-1] + (HEADS, HEAD_DIM))


def pseudo_inverse(landmark_kernel_matrix):
    column_top = jnp.max(jnp.sum(landmark_kernel_matrix, axis=-2), axis=-1)
    row_top = jnp.max(jnp.sum(landmark_kernel_matrix, axis=-1), axis=-1)
    approx = jnp.swapaxes(landmark_kernel_matrix, -1, -2) / (column_top * row_top)[..., None, None]
    ident = jnp.eye(landmark_kernel_matrix.shape[-1], dtype=jnp.float32)
    for turn_index in range(NEWTON):
        product = jnp.matmul(landmark_kernel_matrix, approx, precision=highest_precision)
        inner = 7.0 * ident - product
        inner = 15.0 * ident - jnp.matmul(product, inner, precision=highest_precision)
        inner = 13.0 * ident - jnp.matmul(product, inner, precision=highest_precision)
        approx = 0.25 * jnp.matmul(approx, inner, precision=highest_precision)
    return approx


def landmark_mix(mark_query, mark_key, distant_values):
    scale = HEAD_DIM ** (-0.25)
    scores = jnp.einsum(
        "smhd,snhd->shmn",
        split_heads(mark_query) * scale,
        split_heads(mark_key) * scale,
        precision=highest_precision,
    )
    landmark_kernel_matrix = jax.nn.softmax(scores, axis=-1)
    inverse = pseudo_inverse(landmark_kernel_matrix)
    mixing_result = jnp.matmul(inverse, distant_values, precision=highest_precision)
    ident = jnp.eye(landmark_kernel_matrix.shape[-1], dtype=jnp.float32)
    defect = ident - jnp.matmul(landmark_kernel_matrix, inverse, precision=highest_precision)
    error = jnp.sum(jnp.sqrt(jnp.sum(defect * defect, axis=(-2, -1))))
    return (mixing_result, error)


def near_mix(queries, mark_key, mixing_result, value_ext, taps):
    scale = HEAD_DIM ** (-0.25)
    scores = jnp.einsum(
        NEAR_SCORES,
        split_heads(queries) * scale,
        split_heads(mark_key) * scale,
        precision=highest_precision,
    )
    nearby_part = jax.nn.softmax(scores, axis=-1)
    attended_output = jnp.einsum(
        NEAR_OUT, nearby_part, mixing_result, precision=highest_precision
    )
    window = split_heads(value_ext)
    length = queries.shape[1]
    for tap_index in range(KERNEL):
        attended_output = (
            attended_output
            + taps[:, tap_index][:, None] * window[:, tap_index : tap_index + length]
        )
    return attended_output.reshape(queries.shape)


def far_scores(mark_query, key_rows):
    scale = HEAD_DIM ** (-0.25)
    return jnp.einsum(
        "smhd,sthd->shmt",
        split_heads(mark_query) * scale,
        split_heads(key_rows) * scale,
        precision=highest_precision,
    )


def far_stats(mark_query, key_rows, value_rows):
    scores = far_scores(mark_query, key_rows)
    peak = jnp.max(scores, axis=-1)
    expo = jnp.exp(scores - peak[..., None])
    total = jnp.sum(expo, axis=-1)
    numer = jnp.einsum(
        "shmt,sthd->shmd", expo, split_heads(value_rows), precision=highest_precision
    )
    return (peak, total, numer)


def far_change(mark_query, key_rows, value_rows, peak, total, distant_values):
    expo = jnp.exp(far_scores(mark_query, key_rows) - peak[..., None])
    numer = jnp.einsum(
        "shmt,sthd->shmd", expo, split_heads(value_rows), precision=highest_precision
    )
    return (numer - distant_values * jnp.sum(expo, axis=-1)[..., None]) / total[..., None]


def combine_stats(first, second):
    peak = jnp.maximum(first[0], second[0])
    first_weight = jnp.exp(first[0] - peak)
    second_weight = jnp.exp(second[0] - peak)
    total = first[1] * first_weight + second[1] * second_weight
    numer = first[2] * first_weight[..., None] + second[2] * second_weight[..., None]
    return (peak, total, numer)


def big_product(left, right):
    return jnp.einsum("std,de->ste", left, right, preferred_element_type=jnp.float32)


def weight_grad(left, right):
    return jnp.einsum("std,ste->de", left, right, preferred_element_type=jnp.float32)


def back_product(delta, weight):
    return jnp.einsum("ste,de->std", delta, weight, preferred_element_type=jnp.float32)


def bias_sum(delta):
    return jnp.sum(delta.astype(jnp.float32), axis=(0, 1))


def comm_parts(rows, wide):
    width = FEATURES
    parts = [(at, ALL, ALL) for at in range(4)]
    parts += [(4, ALL, slice(at * width, (at + 1) * width)) for at in range(wide)]
    parts += [(5, slice(at * rows, (at + 1) * rows), ALL) for at in range(wide)]
    return parts + [(6, ALL, ALL)]


def local(
    layer_input,
    query_weight,
    key_weight,
    value_weight,
    output_weight,
    up_weight,
    down_weight,
    query_bias,
    value_bias,
    output_bias,
    up_bias,
    down_bias,
    first_gain,
    first_shift,
    second_gain,
    second_shift,
    mixing_taps,
    output_cotangent,
):
    (
        full_query,
        full_key,
        full_value,
        full_output,
        full_up,
        full_down,
        bias_query,
        bias_value,
        bias_output,
        bias_up,
        bias_down,
        gain_first,
        shift_first,
        gain_second,
        shift_second,
    ) = (
        lax.all_gather(query_weight, BOTH, axis=0, tiled=True),
        lax.all_gather(key_weight, BOTH, axis=0, tiled=True),
        lax.all_gather(value_weight, BOTH, axis=0, tiled=True),
        lax.all_gather(output_weight, BOTH, axis=0, tiled=True),
        lax.all_gather(up_weight, BOTH, axis=0, tiled=True),
        lax.all_gather(down_weight, BOTH, axis=0, tiled=True),
        lax.all_gather(query_bias, BOTH, axis=0, tiled=True),
        lax.all_gather(value_bias, BOTH, axis=0, tiled=True),
        lax.all_gather(output_bias, BOTH, axis=0, tiled=True),
        lax.all_gather(up_bias, BOTH, axis=0, tiled=True),
        lax.all_gather(down_bias, BOTH, axis=0, tiled=True),
        lax.all_gather(first_gain, BOTH, axis=0, tiled=True),
        lax.all_gather(first_shift, BOTH, axis=0, tiled=True),
        lax.all_gather(second_gain, BOTH, axis=0, tiled=True),
        lax.all_gather(second_shift, BOTH, axis=0, tiled=True),
    )
    local_marks = LANDMARKS // lax.axis_size(SEQ)
    batch_rows, tokens, features = layer_input.shape
    segment = tokens // local_marks
    queries = big_product(layer_input, full_query) + bias_query.astype(jnp.float32)
    key_rows = big_product(layer_input, full_key)
    value_rows = (big_product(layer_input, full_value) + bias_value.astype(jnp.float32)).astype(
        jnp.bfloat16
    )
    mark_query = jnp.mean(
        queries.reshape(batch_rows, local_marks, segment, features), axis=2
    ).astype(jnp.bfloat16)
    mark_key = jnp.mean(
        key_rows.reshape(batch_rows, local_marks, segment, features), axis=2
    ).astype(jnp.bfloat16)
    all_query, all_key = (
        lax.all_gather(mark_query, SEQ, axis=1, tiled=True),
        lax.all_gather(mark_key, SEQ, axis=1, tiled=True),
    )
    value_ext = with_halo(value_rows, ((SEQ, 1),), RIM)
    query_marks = all_query.astype(jnp.float32)
    key_marks = all_key.astype(jnp.float32)
    value_float = value_rows.astype(jnp.float32)
    ext_float = value_ext.astype(jnp.float32)
    taps = mixing_taps.astype(jnp.float32)
    stat_peak, stat_total, stat_numer = far_stats(query_marks, key_rows, value_float)
    peak, total, numer = merged((stat_peak, stat_total, stat_numer), SEQ, combine_stats)
    distant_values = numer / total[..., None]
    mixing_result, mix_back, error = jax.vjp(
        landmark_mix, query_marks, key_marks, distant_values, has_aux=True
    )
    attended_output, near_back = jax.vjp(
        near_mix, queries, key_marks, mixing_result, ext_float, taps
    )
    attention = attended_output.astype(jnp.bfloat16)
    resid_first = (
        layer_input.astype(jnp.float32)
        + big_product(attention, full_output)
        + bias_output.astype(jnp.float32)
    )
    hidden, first_back = jax.vjp(
        layer_norm, resid_first, gain_first.astype(jnp.float32), shift_first.astype(jnp.float32)
    )
    hidden_low = hidden.astype(jnp.bfloat16)
    upper = big_product(hidden_low, full_up) + bias_up.astype(jnp.float32)
    activated, gelu_back = jax.vjp(partial(jax.nn.gelu, approximate=False), upper)
    activated_low = activated.astype(jnp.bfloat16)
    resid_second = hidden + big_product(activated_low, full_down) + bias_down.astype(jnp.float32)
    normed, second_back = jax.vjp(
        layer_norm, resid_second, gain_second.astype(jnp.float32), shift_second.astype(jnp.float32)
    )
    layer_output = normed.astype(jnp.bfloat16)
    pinv_error = lax.psum(error, BATCH) / (batch_rows * lax.axis_size(BATCH) * HEADS)
    delta_second, second_gain_grad, second_shift_grad = second_back(
        output_cotangent.astype(jnp.float32)
    )
    delta_lower = delta_second.astype(jnp.bfloat16)
    down_grad = weight_grad(activated_low, delta_lower)
    down_bias_grad = bias_sum(delta_lower)
    delta_upper = gelu_back(back_product(delta_lower, full_down))[0].astype(jnp.bfloat16)
    up_grad = weight_grad(hidden_low, delta_upper)
    up_bias_grad = bias_sum(delta_upper)
    delta_hidden = back_product(delta_upper, full_up) + delta_second
    delta_first, first_gain_grad, first_shift_grad = first_back(delta_hidden)
    delta_proj = delta_first.astype(jnp.bfloat16)
    output_grad = weight_grad(attention, delta_proj)
    output_bias_grad = bias_sum(delta_proj)
    delta_attention = back_product(delta_proj, full_output)
    delta_queries, key_part, mixing_part, delta_ext, taps_part = near_back(delta_attention)
    delta_mixing = jax.tree.map(
        lambda part: part.astype(jnp.float32), lax.psum(for_sending(mixing_part), SEQ)
    )
    query_rep, key_rep, delta_far = mix_back(delta_mixing)
    far_back = jax.vjp(
        partial(far_change, peak=peak, total=total, distant_values=distant_values),
        query_marks,
        key_rows,
        value_float,
    )[1]
    far_query, far_keys, far_vals = far_back(delta_far)
    own_key, own_query = (
        lax.psum_scatter(
            key_part.astype(jnp.bfloat16), SEQ, scatter_dimension=1, tiled=True
        ).astype(jnp.float32),
        lax.psum_scatter(
            far_query.astype(jnp.bfloat16), SEQ, scatter_dimension=1, tiled=True
        ).astype(jnp.float32),
    )
    start = lax.axis_index(SEQ) * local_marks
    own_query = own_query + lax.dynamic_slice_in_dim(query_rep, start, local_marks, 1)
    own_key = own_key + lax.dynamic_slice_in_dim(key_rep, start, local_marks, 1)

    def spread_marks(marks):
        shaped = jnp.broadcast_to(
            (marks / segment)[:, :, None, :], (batch_rows, local_marks, segment, features)
        )
        return shaped.reshape(batch_rows, tokens, features)

    query_delta = (delta_queries + spread_marks(own_query)).astype(jnp.bfloat16)
    key_delta = (far_keys + spread_marks(own_key)).astype(jnp.bfloat16)
    from_left = shifted(for_sending(delta_ext[:, :RIM]), SEQ, -1)
    from_right = shifted(for_sending(delta_ext[:, tokens + RIM :]), SEQ, 1)
    value_sum = delta_ext[:, RIM : RIM + tokens] + far_vals
    value_sum = value_sum + jnp.pad(from_left, ((0, 0), (tokens - RIM, 0), (0, 0)))
    value_sum = value_sum + jnp.pad(from_right, ((0, 0), (0, tokens - RIM), (0, 0)))
    value_delta = value_sum.astype(jnp.bfloat16)
    query_grad = weight_grad(layer_input, query_delta)
    key_grad = weight_grad(layer_input, key_delta)
    value_grad = weight_grad(layer_input, value_delta)
    query_bias_grad = bias_sum(query_delta)
    value_bias_grad = bias_sum(value_delta)
    input_gradient = (
        back_product(query_delta, full_query)
        + back_product(key_delta, full_key)
        + back_product(value_delta, full_value)
        + delta_first
    )
    taps_gradient = lax.psum(taps_part, BOTH)
    owned = (
        lax.psum_scatter(query_grad, BOTH, scatter_dimension=0, tiled=True),
        lax.psum_scatter(key_grad, BOTH, scatter_dimension=0, tiled=True),
        lax.psum_scatter(value_grad, BOTH, scatter_dimension=0, tiled=True),
        lax.psum_scatter(output_grad, BOTH, scatter_dimension=0, tiled=True),
        lax.psum_scatter(up_grad, BOTH, scatter_dimension=0, tiled=True),
        lax.psum_scatter(down_grad, BOTH, scatter_dimension=0, tiled=True),
        lax.psum_scatter(query_bias_grad, BOTH, scatter_dimension=0, tiled=True),
        lax.psum_scatter(value_bias_grad, BOTH, scatter_dimension=0, tiled=True),
        lax.psum_scatter(output_bias_grad, BOTH, scatter_dimension=0, tiled=True),
        lax.psum_scatter(up_bias_grad, BOTH, scatter_dimension=0, tiled=True),
        lax.psum_scatter(down_bias_grad, BOTH, scatter_dimension=0, tiled=True),
        lax.psum_scatter(first_gain_grad, BOTH, scatter_dimension=0, tiled=True),
        lax.psum_scatter(first_shift_grad, BOTH, scatter_dimension=0, tiled=True),
        lax.psum_scatter(second_gain_grad, BOTH, scatter_dimension=0, tiled=True),
        lax.psum_scatter(second_shift_grad, BOTH, scatter_dimension=0, tiled=True),
    )
    return (
        layer_output,
        input_gradient,
        owned[0],
        owned[1],
        owned[2],
        owned[3],
        owned[4],
        owned[5],
        owned[6],
        owned[7],
        owned[8],
        owned[9],
        owned[10],
        owned[11],
        owned[12],
        owned[13],
        owned[14],
        taps_gradient,
        pinv_error,
    )


def exchange_kernel(ways, *refs):
    n = len(ways)
    ins, outs = refs[:n], refs[n : 2 * n]
    send_sem, recv_sem = refs[2 * n :]
    size = lax.axis_size(SEQ)
    batch, me = lax.axis_index(BATCH), lax.axis_index(SEQ)
    barrier = pltpu.get_barrier_semaphore()

    def greet(step, carry):
        peer = lax.rem(me + step, size)
        pl.semaphore_signal(barrier, inc=1, device_id=(batch, peer), device_id_type=MESH)
        return carry

    lax.fori_loop(1, size, greet, 0)
    pl.semaphore_wait(barrier, size - 1)

    def copy_of(at, step):
        peer = lax.rem(me + step, size)
        source = ins[at].at[peer] if ways[at] == SCATTER else ins[at]
        target = outs[at].at[me] if ways[at] in (GATHER, SCATTER) else outs[at]
        return pltpu.make_async_remote_copy(
            src_ref=source,
            dst_ref=target,
            send_sem=send_sem.at[at, step],
            recv_sem=recv_sem.at[at, step],
            device_id=(batch, peer),
            device_id_type=MESH,
        )

    def start(step, carry):
        for at, way in enumerate(ways):
            if way in (GATHER, SCATTER):
                copy_of(at, step).start()
        return carry

    def finish(step, carry):
        for at, way in enumerate(ways):
            if way in (GATHER, SCATTER):
                copy_of(at, step).wait()
        return carry

    single = [(at, {NEXT: 1, LAST: size - 1}[way]) for at, way in enumerate(ways) if way in (NEXT, LAST)]
    for at, step in single:
        copy_of(at, step).start()
    lax.fori_loop(1, size, start, 0)
    for at, way in enumerate(ways):
        if way == GATHER:
            outs[at][me] = ins[at][...]
        elif way == SCATTER:
            outs[at][me] = ins[at][me]
    for at, step in single:
        copy_of(at, step).wait()
    lax.fori_loop(1, size, finish, 0)


def exchange(size, collective_id, *items):
    ways = tuple(way for way, _ in items)
    arrays = [array for _, array in items]
    shapes = [((size,) + a.shape if way == GATHER else a.shape) for way, a in items]
    vmem = pl.BlockSpec(memory_space=pltpu.VMEM)
    return pl.pallas_call(
        partial(exchange_kernel, ways),
        out_shape=[jax.ShapeDtypeStruct(shape, a.dtype) for shape, a in zip(shapes, arrays)],
        in_specs=[vmem] * len(ways),
        out_specs=[vmem] * len(ways),
        scratch_shapes=[
            pltpu.SemaphoreType.DMA((len(ways), size)),
            pltpu.SemaphoreType.DMA((len(ways), size)),
        ],
        compiler_params=pltpu.CompilerParams(collective_id=collective_id, has_side_effects=True),
        name="exchange",
    )(*arrays)


def staged_kernel(batch, seq, ways, *refs):
    n, sums = len(ways), ways.count(SUM)
    ins, outs = refs[:n], refs[n : 2 * n]
    send_sem, recv_sem = refs[-2:]
    scratch = refs[2 * n : -2]
    g = Grid(batch, seq)
    me = lax.axis_index(SEQ)
    ring = {NEXT: lax.rem(me + 1, seq), LAST: lax.rem(me + seq - 1, seq)}
    single = [at for at, way in enumerate(ways) if way in ring]
    barrier = pltpu.get_barrier_semaphore()
    greeted = [g.moved(axis, other) for axis in "zyc" for _, other in g.others(axis)]
    greeted += [(g.at["x"], ring[ways[at]]) for at in single]
    for device in greeted:
        pl.semaphore_signal(barrier, inc=1, device_id=device, device_id_type=MESH)
    pl.semaphore_wait(barrier, len(greeted))
    started = []

    def send(at, stage, step, device, source, target):
        copy = pltpu.make_async_remote_copy(
            src_ref=source,
            dst_ref=target,
            send_sem=send_sem.at[at, stage, step - 1],
            recv_sem=recv_sem.at[at, stage, step - 1],
            device_id=device,
            device_id_type=MESH,
        )
        copy.start()
        started.append(copy)
        return copy

    z, y, c = (g.at[axis] for axis in "zyc")
    alone = [send(at, 0, 1, (g.at["x"], ring[ways[at]]), ins[at], outs[at]) for at in single]
    slots = {at: scratch[4 * rank : 4 * rank + 4] for rank, at in enumerate(a for a, w in enumerate(ways) if w == SUM)}
    for stage in range(3):
        waits = []
        for at, way in enumerate(ways):
            if way == GATHER:
                axis = "zyc"[stage]
                index = ((z, y, c), (ALL, y, c), (ALL, ALL, c))[stage]
                source = ins[at] if stage == 0 else outs[at].at[index]
                for step, other in g.others(axis):
                    waits.append(send(at, stage, step, g.moved(axis, other), source, outs[at].at[index]))
                if stage == 0:
                    outs[at][index] = ins[at][...]
            elif way == SUM:
                held, *came = slots[at]
                axis = "cyz"[stage]
                for step, other in g.others(axis):
                    source = (
                        lambda: ins[at].at[:, :, other],
                        lambda: held.at[:, other],
                        lambda: held.at[other, y],
                    )[stage]()
                    target = came[stage].at[step - 1] if stage == 2 else came[stage]
                    waits.append(send(at, stage, step, g.moved(axis, other), source, target))
        for copy in waits:
            copy.wait_recv()
        for at in slots:
            held, from_core, from_far, from_line = slots[at]
            wide = jnp.float32
            if stage == 0:
                total = ins[at][:, :, c].astype(wide) + from_core[...].astype(wide)
                held[...] = total.astype(held.dtype)
            elif stage == 1:
                total = held[:, y].astype(wide) + from_far[...].astype(wide)
                held[:, y] = total.astype(held.dtype)
            else:
                total = held[z, y].astype(wide)
                for step, _ in g.others("z"):
                    total += from_line[step - 1].astype(wide)
                outs[at][...] = total
    for copy in alone:
        copy.wait_recv()
    for copy in started:
        copy.wait_send()


def staged(batch, seq, collective_id, *items):
    _, nz, ny, nc = grid_of(batch, seq)
    ways = tuple(way for way, _ in items)
    arrays = [a.reshape((nz, ny, nc) + a.shape[1:]) if way == SUM else a for way, a in items]
    shapes, scratch = [], []
    for way, a in zip(ways, arrays):
        shape, kind = a.shape, a.dtype
        if way == GATHER:
            shape = (nz, ny, nc) + shape
        elif way == SUM:
            shape, kind = shape[3:], jnp.float32
            scratch += [
                pltpu.VMEM((nz, ny) + shape, a.dtype),
                pltpu.VMEM((nz, ny) + shape, a.dtype),
                pltpu.VMEM((nz,) + shape, a.dtype),
                pltpu.VMEM((nz - 1,) + shape, a.dtype),
            ]
        shapes.append(jax.ShapeDtypeStruct(shape, kind))
    vmem = pl.BlockSpec(memory_space=pltpu.VMEM)
    results = pl.pallas_call(
        partial(staged_kernel, batch, seq, ways),
        out_shape=shapes,
        in_specs=[vmem] * len(ways),
        out_specs=[vmem] * len(ways),
        scratch_shapes=scratch
        + [
            pltpu.SemaphoreType.DMA((len(ways), 3, nz - 1)),
            pltpu.SemaphoreType.DMA((len(ways), 3, nz - 1)),
        ],
        compiler_params=pltpu.CompilerParams(collective_id=collective_id, has_side_effects=True),
        name="staged",
    )(*arrays)
    return [
        r.reshape((seq,) + r.shape[3:]) if way == GATHER else r for way, r in zip(ways, results)
    ]


def own_mix(mark_query, mark_key, distant_values):
    scale = HEAD_DIM ** (-0.25)
    heads = distant_values.shape[0]

    def pair(marks):
        return marks.reshape(marks.shape[0], heads, HEAD_DIM) * scale

    scores = jnp.einsum("mhd,nhd->hmn", pair(mark_query), pair(mark_key), precision=highest_precision)
    landmark_kernel_matrix = jax.nn.softmax(scores, axis=-1)
    inverse = pseudo_inverse(landmark_kernel_matrix)
    mixing_result = jnp.matmul(inverse, distant_values, precision=highest_precision)
    ident = jnp.eye(landmark_kernel_matrix.shape[-1], dtype=jnp.float32)
    defect = ident - jnp.matmul(landmark_kernel_matrix, inverse, precision=highest_precision)
    error = jnp.sum(jnp.sqrt(jnp.sum(defect * defect, axis=(-2, -1))))
    return (mixing_result, error)


def far_back(mark_query, key_rows, value_rows, peak, total, delta_far, inner):
    scale = HEAD_DIM ** (-0.25)
    near_one = jnp.exp(far_scores(mark_query, key_rows) - peak[..., None]) / total[..., None]
    values = split_heads(value_rows)
    far_vals = jnp.einsum("shmt,shmd->sthd", near_one, delta_far, precision=highest_precision)
    slope = jnp.einsum("shmd,sthd->shmt", delta_far, values, precision=highest_precision)
    slope = near_one * (slope - inner[..., None])
    far_query = jnp.einsum("shmt,sthd->smhd", slope, split_heads(key_rows) * scale, precision=highest_precision)
    far_keys = jnp.einsum("shmt,smhd->sthd", slope, split_heads(mark_query) * scale, precision=highest_precision)
    return (
        (far_query * scale).reshape(mark_query.shape),
        (far_keys * scale).reshape(key_rows.shape),
        far_vals.reshape(value_rows.shape),
    )


def near_mix_banded(queries, mark_key, mixing_result, value_ext, taps):
    scale = HEAD_DIM ** (-0.25)
    scores = jnp.einsum(
        NEAR_SCORES, split_heads(queries) * scale, split_heads(mark_key) * scale, precision=highest_precision
    )
    nearby_part = jax.nn.softmax(scores, axis=-1)
    attended_output = jnp.einsum(NEAR_OUT, nearby_part, mixing_result, precision=highest_precision)
    length, reach = queries.shape[1], value_ext.shape[1]
    shape = (KERNEL, length, reach)
    tap, token, source = (lax.broadcasted_iota(jnp.int32, shape, at) for at in range(3))
    chosen = (source - token == tap).astype(jnp.float32)
    banded = jnp.einsum("hj,jtu->htu", taps, chosen, precision=highest_precision)
    attended_output = attended_output + jnp.einsum(
        "htu,suhd->sthd", banded, split_heads(value_ext), precision=highest_precision
    )
    return attended_output.reshape(queries.shape)


def local_fast(
    batch,
    seq,
    layer_input,
    query_weight,
    key_weight,
    value_weight,
    output_weight,
    up_weight,
    down_weight,
    query_bias,
    value_bias,
    output_bias,
    up_bias,
    down_bias,
    first_gain,
    first_shift,
    second_gain,
    second_shift,
    mixing_taps,
    output_cotangent,
):
    weights = (query_weight, key_weight, value_weight, output_weight, up_weight, down_weight)
    vectors = (
        query_bias,
        value_bias,
        output_bias,
        down_bias,
        first_gain,
        first_shift,
        second_gain,
        second_shift,
    )
    own = query_bias.shape[0]
    wide = up_bias.shape[0] // own
    packed = jnp.concatenate([*(v[None] for v in vectors), up_bias.reshape(wide, own)], axis=0)
    packed = jnp.pad(packed, ((0, 16 - packed.shape[0]), (0, 128 - own)))
    parts = comm_parts(own, wide)
    orders = ["xy" if at % 2 == 0 else "yx" for at in range(len(parts))]
    *gathered, vectors_all = gather_weights(
        batch, seq, weights + (packed,), parts, orders, 2, 1
    )
    full_query, full_key, full_value, full_output, full_up, full_down = (
        whole.reshape(-1, whole.shape[-1]) for whole in gathered
    )
    table = jnp.swapaxes(vectors_all.reshape(batch * seq, 16, 128)[:, :, :own], 0, 1)
    (
        bias_query,
        bias_value,
        bias_output,
        bias_down,
        gain_first,
        shift_first,
        gain_second,
        shift_second,
    ) = (table[at].reshape(-1) for at in range(8))
    bias_up = jnp.swapaxes(table[8 : 8 + wide], 0, 1).reshape(-1)
    local_marks = LANDMARKS // lax.axis_size(SEQ)
    batch_rows, tokens, features = layer_input.shape
    segment = tokens // local_marks
    queries = big_product(layer_input, full_query) + bias_query.astype(jnp.float32)
    key_rows = big_product(layer_input, full_key)
    value_rows = (big_product(layer_input, full_value) + bias_value.astype(jnp.float32)).astype(
        jnp.bfloat16
    )
    mark_query = jnp.mean(
        queries.reshape(batch_rows, local_marks, segment, features), axis=2
    ).astype(jnp.bfloat16)
    mark_key = jnp.mean(
        key_rows.reshape(batch_rows, local_marks, segment, features), axis=2
    ).astype(jnp.bfloat16)
    marks, before, after = staged(
        batch,
        seq,
        3,
        (GATHER, jnp.stack([mark_query, mark_key]).reshape(-1, features)),
        (NEXT, value_rows[:, tokens - RIM :]),
        (LAST, value_rows[:, :RIM]),
    )
    place_at = lax.axis_index(SEQ)
    before = jnp.where(place_at > 0, before, jnp.zeros_like(before))
    after = jnp.where(place_at < seq - 1, after, jnp.zeros_like(after))
    value_ext = jnp.concatenate([before, value_rows, after], axis=1)
    marks = marks.reshape(seq, 2, batch_rows, local_marks, features)
    marks = jnp.transpose(marks, (1, 2, 0, 3, 4)).reshape(2, batch_rows, LANDMARKS, features)
    query_marks, key_marks = marks[0].astype(jnp.float32), marks[1].astype(jnp.float32)
    value_float = value_rows.astype(jnp.float32)
    ext_float = value_ext.astype(jnp.float32)
    taps = mixing_taps.astype(jnp.float32)
    stat_peak, stat_total, stat_numer = far_stats(query_marks, key_rows, value_float)
    owners = batch_rows * HEADS // 2
    low = jnp.bfloat16

    def to_owners(matrices):
        pairs = matrices.reshape(owners, 2, LANDMARKS, HEAD_DIM).astype(low)
        pairs = jnp.swapaxes(pairs, 1, 2).reshape(owners, LANDMARKS, 2 * HEAD_DIM)
        return jnp.concatenate([pairs, pairs[: seq - owners]], axis=0)

    def as_pair(sides):
        return jnp.swapaxes(sides.reshape(LANDMARKS, 2, HEAD_DIM), 0, 1)

    def as_sides(pair):
        return jnp.swapaxes(pair, 0, 1).reshape(LANDMARKS, 2 * HEAD_DIM)

    def from_owners(sides):
        pairs = sides[:owners].reshape(owners, LANDMARKS, 2, HEAD_DIM).astype(jnp.float32)
        return jnp.swapaxes(pairs, 1, 2).reshape(batch_rows, HEADS, LANDMARKS, HEAD_DIM)

    def rows_to_owners(*rows):
        table = jnp.stack([row.reshape(owners, 2 * LANDMARKS) for row in rows], axis=1)
        table = jnp.pad(table, ((0, 0), (0, 8 - len(rows)), (0, 0)))
        return jnp.concatenate([table, table[: seq - owners]], axis=0)

    def rows_from_owners(table, at):
        return table[:owners, at].reshape(batch_rows, HEADS, LANDMARKS)

    numers, stats = exchange(
        seq,
        4,
        (SCATTER, to_owners(stat_numer)),
        (SCATTER, rows_to_owners(stat_peak, stat_total)),
    )
    peak_rows, total_rows = stats[:, 0], stats[:, 1]
    peak_own = jnp.max(peak_rows, axis=0)
    weights_own = jnp.exp(peak_rows - peak_own)
    total_own = jnp.sum(total_rows * weights_own, axis=0)
    numer_pairs = jnp.swapaxes(numers.astype(jnp.float32).reshape(seq, LANDMARKS, 2, HEAD_DIM), 1, 2)
    shares = (weights_own / total_own).reshape(seq, 2, LANDMARKS, 1)
    distant_own = jnp.sum(numer_pairs * shares, axis=0)
    owner = lax.rem(place_at, owners)
    own_row, own_lane = owner // (HEADS // 2), (owner % (HEADS // 2)) * 2 * HEAD_DIM

    def own_marks(all_marks):
        return lax.dynamic_slice(all_marks, (own_row, 0, own_lane), (1, LANDMARKS, 2 * HEAD_DIM))[0]

    mixing_own, mix_back, error = jax.vjp(
        own_mix, own_marks(query_marks), own_marks(key_marks), distant_own, has_aux=True
    )
    mixings, stats = staged(
        batch,
        seq,
        5,
        (GATHER, as_sides(mixing_own).astype(low)),
        (GATHER, jnp.pad(jnp.stack([peak_own, total_own]), ((0, 6), (0, 0)))),
    )
    mixing_result = from_owners(mixings)
    peak, total = rows_from_owners(stats, 0), rows_from_owners(stats, 1)
    attended_output, near_back = jax.vjp(
        near_mix_banded, queries, key_marks, mixing_result, ext_float, taps
    )
    attention = attended_output.astype(jnp.bfloat16)
    resid_first = (
        layer_input.astype(jnp.float32)
        + big_product(attention, full_output)
        + bias_output.astype(jnp.float32)
    )
    hidden, first_back = jax.vjp(
        layer_norm, resid_first, gain_first.astype(jnp.float32), shift_first.astype(jnp.float32)
    )
    hidden_low = hidden.astype(jnp.bfloat16)
    upper = big_product(hidden_low, full_up) + bias_up.astype(jnp.float32)
    activated, gelu_back = jax.vjp(partial(jax.nn.gelu, approximate=False), upper)
    activated_low = activated.astype(jnp.bfloat16)
    resid_second = hidden + big_product(activated_low, full_down) + bias_down.astype(jnp.float32)
    normed, second_back = jax.vjp(
        layer_norm, resid_second, gain_second.astype(jnp.float32), shift_second.astype(jnp.float32)
    )
    layer_output = normed.astype(jnp.bfloat16)
    delta_second, second_gain_grad, second_shift_grad = second_back(
        output_cotangent.astype(jnp.float32)
    )
    delta_lower = delta_second.astype(jnp.bfloat16)
    down_grad = weight_grad(activated_low, delta_lower)
    down_bias_grad = bias_sum(delta_lower)
    delta_upper = gelu_back(back_product(delta_lower, full_down))[0].astype(jnp.bfloat16)
    up_grad = weight_grad(hidden_low, delta_upper)
    up_bias_grad = bias_sum(delta_upper)
    delta_hidden = back_product(delta_upper, full_up) + delta_second
    delta_first, first_gain_grad, first_shift_grad = first_back(delta_hidden)
    delta_proj = delta_first.astype(jnp.bfloat16)
    output_grad = weight_grad(attention, delta_proj)
    output_bias_grad = bias_sum(delta_proj)
    delta_attention = back_product(delta_proj, full_output)
    delta_queries, key_part, mixing_part, delta_ext, taps_part = near_back(delta_attention)
    (parts_own,) = staged(batch, seq, 6, (SUM, to_owners(mixing_part)))
    delta_mixing = as_pair(parts_own)
    query_own, key_own, far_own = mix_back(delta_mixing)
    inner_own = jnp.sum(far_own * distant_own, axis=-1).reshape(1, 2 * LANDMARKS)
    delta_fars, inners = staged(
        batch,
        seq,
        7,
        (GATHER, as_sides(far_own).astype(low)),
        (GATHER, jnp.pad(inner_own, ((0, 7), (0, 0)))),
    )
    far_query, far_keys, far_vals = far_back(
        query_marks, key_rows, value_float, peak, total, from_owners(delta_fars), rows_from_owners(inners, 0)
    )
    active = jnp.where(place_at < owners, 1.0, 0.0)

    def with_own(part, own):
        at = (own_row, 0, own_lane)
        held = lax.dynamic_slice(part, at, (1, LANDMARKS, 2 * HEAD_DIM))
        return lax.dynamic_update_slice(part, held + active * own[None], at)

    def by_owner(part):
        return jnp.swapaxes(part.reshape(batch_rows, seq, local_marks, features), 0, 1).astype(low)

    spread = jnp.stack(
        [by_owner(with_own(far_query, query_own)), by_owner(with_own(key_part, key_own))], axis=1
    )
    marks_parts, from_right, from_left = staged(
        batch,
        seq,
        8,
        (SUM, spread.reshape(seq, -1, features)),
        (LAST, for_sending(delta_ext[:, :RIM])),
        (NEXT, for_sending(delta_ext[:, tokens + RIM :])),
    )
    from_right = jnp.where(place_at < seq - 1, from_right, jnp.zeros_like(from_right))
    from_left = jnp.where(place_at > 0, from_left, jnp.zeros_like(from_left))
    own_query, own_key = marks_parts.reshape(2, batch_rows, local_marks, features)

    def spread_marks(marks):
        shaped = jnp.broadcast_to(
            (marks / segment)[:, :, None, :], (batch_rows, local_marks, segment, features)
        )
        return shaped.reshape(batch_rows, tokens, features)

    query_delta = (delta_queries + spread_marks(own_query)).astype(jnp.bfloat16)
    key_delta = (far_keys + spread_marks(own_key)).astype(jnp.bfloat16)
    value_sum = delta_ext[:, RIM : RIM + tokens] + far_vals
    value_sum = value_sum + jnp.pad(from_right, ((0, 0), (tokens - RIM, 0), (0, 0)))
    value_sum = value_sum + jnp.pad(from_left, ((0, 0), (0, tokens - RIM), (0, 0)))
    value_delta = value_sum.astype(jnp.bfloat16)
    query_grad = weight_grad(layer_input, query_delta)
    key_grad = weight_grad(layer_input, key_delta)
    value_grad = weight_grad(layer_input, value_delta)
    query_bias_grad = bias_sum(query_delta)
    value_bias_grad = bias_sum(value_delta)
    input_gradient = (
        back_product(query_delta, full_query)
        + back_product(key_delta, full_key)
        + back_product(value_delta, full_value)
        + delta_first
    )
    error_share = jnp.where(place_at < owners, error, 0.0) / (batch_rows * batch * HEADS)
    joined = jnp.concatenate([taps_part.reshape(-1), error_share[None]])
    joined = jnp.pad(joined, (0, 4 * 128 - joined.shape[0])).reshape(1, 4, 128)
    sizes = grid_of(batch, seq)
    grads = [
        grad.astype(jnp.bfloat16).reshape(sizes + (-1, grad.shape[-1]))
        for grad in (query_grad, key_grad, value_grad, output_grad, up_grad, down_grad)
    ]
    rows = [
        query_bias_grad,
        value_bias_grad,
        output_bias_grad,
        down_bias_grad,
        first_gain_grad,
        first_shift_grad,
        second_gain_grad,
        second_shift_grad,
    ]
    sums = jnp.concatenate(
        [
            jnp.swapaxes(jnp.stack(rows).reshape(8, batch * seq, own), 0, 1),
            up_bias_grad.reshape(batch * seq, wide, own),
        ],
        axis=1,
    )
    sums = jnp.pad(sums, ((0, 0), (0, 0), (0, 128 - own)))
    sums = jnp.concatenate([sums, jnp.broadcast_to(joined, (batch * seq, 4, 128))], axis=1)
    *owned, mine = scatter_grads(
        batch, seq, grads + [sums.reshape(sizes + (16, 128))], parts, orders, 2, 2
    )
    joined = mine[12:].reshape(-1)
    taps_gradient = joined[: HEADS * KERNEL].reshape(taps_part.shape)
    pinv_error = joined[HEADS * KERNEL]
    owned += [mine[0, :own], mine[1, :own], mine[2, :own], mine[8 : 8 + wide, :own].reshape(-1)]
    owned += [mine[at, :own] for at in range(3, 8)]
    return (
        layer_output,
        input_gradient,
        owned[0],
        owned[1],
        owned[2],
        owned[3],
        owned[4],
        owned[5],
        owned[6],
        owned[7],
        owned[8],
        owned[9],
        owned[10],
        owned[11],
        owned[12],
        owned[13],
        owned[14],
        taps_gradient,
        pinv_error,
    )


def solution(mesh):
    placed = (
        TOKENS,
        ROWS,
        ROWS,
        ROWS,
        ROWS,
        ROWS,
        ROWS,
        SPREAD,
        SPREAD,
        SPREAD,
        SPREAD,
        SPREAD,
        SPREAD,
        SPREAD,
        SPREAD,
        SPREAD,
        P(),
        TOKENS,
    )
    batch, seq = mesh.shape[BATCH], mesh.shape[SEQ]
    fits = seq == 16 and FEATURES % (8 * batch * seq) == 0
    return jax.shard_map(
        partial(local_fast, batch, seq) if fits else local,
        mesh=mesh,
        in_specs=placed,
        out_specs=(
            TOKENS,
            TOKENS,
            ROWS,
            ROWS,
            ROWS,
            ROWS,
            ROWS,
            ROWS,
            SPREAD,
            SPREAD,
            SPREAD,
            SPREAD,
            SPREAD,
            SPREAD,
            SPREAD,
            SPREAD,
            SPREAD,
            P(),
            P(),
        ),
        check_vma=False,
    )
```
